16 devices in a mesh: data: 2 (over y, z), expert: 8 (over x, core).
Axes of the slice: x: 4, y: 2, z: 1, core: 2. Of those that a mesh axis runs over, the one named last changes fastest.
The devices are a block of a 4x4x8 slice.
Arguments:
- x_a: bfloat16 [2048, 2048], P(('data', 'expert')), parts along dimension 0
- idx_a: int32 [2048, 6], P(('data', 'expert')), parts along dimension 0
- gate_a: float32 [2048, 6], P(('data', 'expert')), parts along dimension 0
- x_b: bfloat16 [2048, 2048], P(('data', 'expert')), parts along dimension 0
- idx_b: int32 [2048, 6], P(('data', 'expert')), parts along dimension 0
- gate_b: float32 [2048, 6], P(('data', 'expert')), parts along dimension 0
- w_up: bfloat16 [64, 2048, 1408], P('expert')
- w_down: bfloat16 [64, 1408, 2048], P('expert')
Outputs:
- output 1: bfloat16 [2048, 2048], P(('data', 'expert')), parts along dimension 0
- output 2: bfloat16 [2048, 2048], P(('data', 'expert')), parts along dimension 0
There are 2 independent parts. The reference program is written for one: setup_inputs(seed, part) draws one part's arguments, and reference() takes and returns one part's arrays. A program takes and returns all parts, laid end to end along the dimension named above; an argument that names none is the same for every part.
All inputs are finite; a program needn't handle non-finite values.
Results may differ from the reference program's by a relative error of at most 0.00553068.
Values are sent between devices in bfloat16 or wider.
A program may use at most 768 MiB of HBM per device.

```python
import jax
import jax.numpy as jnp
from jax import lax

TOKENS_DEV = 128
GROUP_SIZE = 8
MODEL_DIM = 2048
FFN_DIM = 1408
EXPERTS = 64
TOP_K = 6
CAPACITY = 96


def draw_routing(rng_key):
    mean_load = TOKENS_DEV * TOP_K // EXPERTS
    half_count = EXPERTS // 2
    key_perm, key_devs = jax.random.split(rng_key)
    relabel = jax.random.permutation(key_perm, EXPERTS)
    dev_keys = jax.random.split(key_devs, GROUP_SIZE)

    def one_device(dev_key):
        sub_keys = jax.random.split(dev_key, 5)
        pair_shift = jax.random.randint(sub_keys[0], (half_count,), 0, mean_load + 1)
        full_pair = jax.random.randint(sub_keys[1], (), 0, half_count)
        pair_shift = jnp.where(jnp.arange(half_count) == full_pair, mean_load, pair_shift)
        pair_flip = jnp.where(jax.random.randint(sub_keys[2], (half_count,), 0, 4) < 3, 1, -1)
        pair_counts = jnp.stack([mean_load + pair_flip * pair_shift, mean_load - pair_flip * pair_shift], axis=1).reshape(EXPERTS)
        dev_counts = jnp.zeros((EXPERTS,), jnp.int32).at[relabel].set(pair_counts)
        range_ends = jnp.cumsum(dev_counts)
        sorted_ids = jnp.searchsorted(range_ends, jnp.arange(TOKENS_DEV * TOP_K), side='right')
        choice_tab = sorted_ids.reshape(TOP_K, TOKENS_DEV).T
        choice_tab = choice_tab[jax.random.permutation(sub_keys[3], TOKENS_DEV)]
        rot_rows = jax.random.randint(sub_keys[4], (TOKENS_DEV, 1), 0, TOP_K)
        col_ids = (jnp.arange(TOP_K)[None, :] + rot_rows) % TOP_K
        return jnp.take_along_axis(choice_tab, col_ids, axis=1).astype(jnp.int32)

    return jax.vmap(one_device)(dev_keys).reshape(GROUP_SIZE * TOKENS_DEV, TOP_K)


def setup_inputs(seed: int = 0, part: int = 0) -> dict:
    part_keys = jax.random.split(jax.random.fold_in(jax.random.key(seed), part), 6)
    weight_keys = jax.random.split(jax.random.key(seed + 1), 2)
    n_rows = GROUP_SIZE * TOKENS_DEV
    gate_scale = TOP_K ** -0.5
    x_a = jax.random.normal(part_keys[0], (n_rows, MODEL_DIM), jnp.float32).astype(jnp.bfloat16)
    idx_a = draw_routing(part_keys[1])
    gate_a = jax.random.uniform(part_keys[2], (n_rows, TOP_K), jnp.float32, 0.5, 1.5) * gate_scale
    x_b = jax.random.normal(part_keys[3], (n_rows, MODEL_DIM), jnp.float32).astype(jnp.bfloat16)
    idx_b = draw_routing(part_keys[4])
    gate_b = jax.random.uniform(part_keys[5], (n_rows, TOP_K), jnp.float32, 0.5, 1.5) * gate_scale
    w_up = (jax.random.normal(weight_keys[0], (EXPERTS, MODEL_DIM, FFN_DIM), jnp.float32) * MODEL_DIM ** -0.5).astype(jnp.bfloat16)
    w_down = (jax.random.normal(weight_keys[1], (EXPERTS, FFN_DIM, MODEL_DIM), jnp.float32) * FFN_DIM ** -0.5).astype(jnp.bfloat16)
    return dict(x_a=x_a, idx_a=idx_a, gate_a=gate_a, x_b=x_b, idx_b=idx_b, gate_b=gate_b, w_up=w_up, w_down=w_down)


def moe_layer(tok_rows, route_ids, gate_vals, w_up, w_down):
    n_rows = GROUP_SIZE * TOKENS_DEV
    n_pairs = n_rows * TOP_K
    flat_ids = route_ids.reshape(n_pairs)
    sort_order = jnp.argsort(flat_ids, stable=True)
    counts = jnp.zeros((EXPERTS,), jnp.int32).at[flat_ids].add(1)
    starts = jnp.cumsum(counts) - counts
    sorted_rank = jnp.arange(n_pairs, dtype=jnp.int32) - starts[flat_ids[sort_order]]
    slot_rank = jnp.zeros((n_pairs,), jnp.int32).at[sort_order].set(sorted_rank)
    slot_index = jnp.where(slot_rank < CAPACITY, flat_ids * CAPACITY + slot_rank, EXPERTS * CAPACITY)
    pair_token = jnp.arange(n_pairs, dtype=jnp.int32) // TOP_K
    buffer = jnp.zeros((EXPERTS * CAPACITY, MODEL_DIM), jnp.bfloat16).at[slot_index].set(tok_rows[pair_token], mode='drop')

    def expert_ffn(operands):
        rows_in, up_mat, down_mat = operands
        hidden = jax.nn.gelu(jnp.dot(rows_in, up_mat, preferred_element_type=jnp.float32)).astype(jnp.bfloat16)
        return jnp.dot(hidden, down_mat, preferred_element_type=jnp.float32).astype(jnp.bfloat16)

    expert_out = lax.map(expert_ffn, (buffer.reshape(EXPERTS, CAPACITY, MODEL_DIM), w_up, w_down))
    pair_out = jnp.take(expert_out.reshape(EXPERTS * CAPACITY, MODEL_DIM), slot_index, axis=0, mode='fill', fill_value=0)
    pair_out = pair_out.astype(jnp.float32).reshape(n_rows, TOP_K, MODEL_DIM)
    mix_sum = jnp.sum(gate_vals[:, :, None] * pair_out, axis=1)
    return (tok_rows.astype(jnp.float32) + mix_sum).astype(jnp.bfloat16)


def reference(x_a, idx_a, gate_a, x_b, idx_b, gate_b, w_up, w_down):
    y_a = moe_layer(x_a, idx_a, gate_a, w_up, w_down)
    y_b = moe_layer(x_b, idx_b, gate_b, w_up, w_down)
    return (y_a, y_b)
```

```python
import functools

import jax
import jax.numpy as jnp
from jax import lax
from jax.experimental import pallas as pl
from jax.experimental.pallas import tpu as pltpu
from jax.sharding import PartitionSpec as P

F32 = jnp.float32
BF16 = jnp.bfloat16
CW = 256
TW = 512


def moe_kernel(dims, idx_a, gate_a, idx_b, gate_b, xa_hbm, xb_hbm, wu_hbm, wd_hbm, ya_hbm, yb_hbm,
               xall, buf, hid, w1, w2, coef, pick, pick_f, meta, osum, part, dbuf, cbuf, rbuf, fbuf, ybuf,
               meta_send, meta_recv, x_sem, ag_send, ag_recv, fwd_send, core_send, core_recv,
               w1_sem, w2_sem, d_send, d_recv, r_send, r_recv, f_send, f_recv, y_sem):
    n_dev, n_chip, tok, k_top, d_model, d_ff, n_exp, load, cap = dims
    lanes = coef.shape[-1]
    rows = n_dev * load
    half = tok // 2
    pair = 2 * load
    n_col = d_model // CW
    n_step = 2 * n_col
    bounds = [(t, min(TW, d_ff - t)) for t in range(0, d_ff, TW)]
    n_tile = len(bounds)
    n_slot_p, n_slot_d, n_slot_f = part.shape[0], dbuf.shape[0], fbuf.shape[0]
    e_half = n_exp // 2
    n_slot_w2 = w2.shape[0]

    me = lax.axis_index('expert')
    chip, core = me // 2, lax.rem(me, 2)
    other = 1 - core
    right_c, left_c, far_c = lax.rem(chip + 1, n_chip), lax.rem(chip + n_chip - 1, n_chip), lax.rem(chip + 2, n_chip)
    partner = chip * 2 + other
    side = (right_c * 2 + core, left_c * 2 + core)

    def remote(src, dst, send, recv, dev):
        return pltpu.make_async_remote_copy(src_ref=src, dst_ref=dst, send_sem=send, recv_sem=recv,
                                            device_id={'expert': dev}, device_id_type=pl.DeviceIdType.MESH)

    def w1_copy(e, t):
        lo, width = bounds[t]
        return pltpu.make_async_copy(wu_hbm.at[e, :, pl.ds(lo, width)], w1.at[t, :, pl.ds(0, width)], w1_sem.at[t])

    def w2_copy(q):
        step, part_id = q // 2, lax.rem(q, 2)
        col = pl.multiple_of(lax.rem(step, n_col) * CW, CW)
        slot = lax.rem(q, n_slot_w2)
        return pltpu.make_async_copy(wd_hbm.at[pl.ds(part_id * e_half, e_half), :, pl.ds(col, CW)], w2.at[slot], w2_sem.at[slot])

    def block(m, c, r0=0, n=tok, k=None):
        k = core if k is None else k
        return xall.at[m, c, pl.ds(pl.multiple_of(k * tok + r0, 16), n), :]

    def own_load(m):
        return pltpu.make_async_copy((xa_hbm, xb_hbm)[m], block(m, chip), x_sem.at[m])

    def own_send(m, d, h):
        ref = block(m, chip, h * half, half)
        return remote(ref, ref, ag_send.at[m, d, h], ag_recv.at[m, d, h], side[d])

    def own_arrival(m, d, h):
        ref = block(m, (left_c, right_c)[d], h * half, half)
        return remote(ref, ref, ag_send.at[m, d, h], ag_recv.at[m, d, h], side[d])

    def forward(m, d):
        ref = block(m, (left_c, right_c)[d], d * half, half)
        return remote(ref, ref, fwd_send.at[m, d], ag_recv.at[m, d, 2], side[d])

    def far_arrival(m, d):
        ref = block(m, far_c, d * half, half)
        return remote(ref, ref, fwd_send.at[m, d], ag_recv.at[m, d, 2], side[d])

    def to_partner(m, i):
        ref = block(m, (chip, right_c, left_c, far_c)[i])
        return remote(ref, ref, core_send.at[m, i], core_recv.at[m, i], partner)

    def from_partner(m, i):
        ref = block(m, (chip, right_c, left_c, far_c)[i], k=other)
        return remote(ref, ref, core_send.at[m, i], core_recv.at[m, i], partner)

    def start_own(m):
        own_send(m, 0, 0).start()
        own_send(m, 1, 1).start()
        own_send(m, 0, 1).start()
        own_send(m, 1, 0).start()
        to_partner(m, 0).start()

    def relay_first(m):
        for d in range(2):
            own_arrival(m, d, d).wait_recv()
            forward(m, d).start()

    def relay_second(m):
        own_arrival(m, 1, 0).wait_recv()
        to_partner(m, 1).start()
        own_arrival(m, 0, 1).wait_recv()
        to_partner(m, 2).start()

    def relay_far(m):
        for d in range(2):
            far_arrival(m, d).wait_recv()
        to_partner(m, 3).start()

    def routing(m):
        lane = lax.broadcasted_iota(jnp.int32, (1, lanes), 1)
        lane_e = jnp.where(lane < n_exp * load, me * n_exp + lane // load, -1).astype(F32)
        lane_r = lax.rem(lane, load).astype(F32)
        row_id = lax.broadcasted_iota(jnp.int32, (tok, tok), 0)
        col_id = lax.broadcasted_iota(jnp.int32, (tok, tok), 1)
        below = jnp.where(col_id < row_id, 1.0, 0.0).astype(BF16)

        def one_source(s, before):
            facts = jnp.concatenate([meta[s], jnp.zeros((tok - meta.shape[1], tok), F32)], axis=0).T
            hit = jnp.zeros((tok, lanes), F32)
            gate = jnp.zeros((tok, lanes), F32)
            for j in range(k_top):
                same = facts[:, 16 * m + j:16 * m + j + 1] == lane_e
                hit = jnp.where(same, 1.0, hit)
                gate = jnp.where(same, facts[:, 16 * m + 8 + j:16 * m + 9 + j], gate)
            rank = jnp.dot(below, hit.astype(BF16), preferred_element_type=F32)
            keep = (hit > 0.0) & (rank == lane_r) & (before + rank < float(cap))
            gate = jnp.where(keep, gate, 0.0)
            hi = (gate * 0.9921875).astype(BF16)
            rest = gate - hi.astype(F32)
            mid = rest.astype(BF16)
            low = (rest - mid.astype(F32)).astype(BF16)
            coef[m, 0, s] = hi
            coef[m, 1, s] = mid
            coef[m, 2, s] = low
            chosen = jnp.where(keep, 1.0, 0.0).T
            return before + jnp.sum(hit, axis=0, keepdims=True), chosen

        before = jnp.zeros((1, lanes), F32)
        for c in range(n_chip):
            for k in range(2):
                before, chosen = one_source(2 * c + k, before)
                for e in range(n_exp):
                    pick_f[e * pair + k * load:e * pair + (k + 1) * load, k * tok:(k + 1) * tok] = chosen[e * load:(e + 1) * load]
            pick[m, c] = pick_f[...].astype(BF16)

    def gather(m, c):
        for n in range(0, d_model, 512):
            got = jnp.dot(pick[m, c], xall[m, c, :, n:n + 512], preferred_element_type=F32).astype(BF16)
            for e in range(n_exp):
                buf[e, pl.ds(pl.multiple_of(c * pair, 16), pair), n:n + 512] = got[e * pair:(e + 1) * pair]

    def up(m, e):
        for t, (lo, width) in enumerate(bounds):
            w1_copy(e, t).wait()
            acc = jnp.dot(buf[e], w1[t, :, 0:width], preferred_element_type=F32)
            hid[m, e, :, lo:lo + width] = jax.nn.gelu(acc, approximate=True).astype(BF16)
            nxt = m * n_exp + e + 1

            @pl.when(nxt < 2 * n_exp)
            def _():
                w1_copy(lax.rem(nxt, n_exp), t).start()

    def down(m, k):
        slot = lax.rem(k, n_slot_p)
        for p in range(2):
            q = 2 * k + p
            w2_copy(q).wait()
            for i in range(e_half):
                e = p * e_half + i
                out = jnp.dot(hid[m, e], w2[lax.rem(q, n_slot_w2), i], preferred_element_type=F32)
                for s in range(n_dev):
                    osum[s, e * load:(e + 1) * load, :] = out[s * load:(s + 1) * load]

            @pl.when(q + n_slot_w2 < 2 * n_step)
            def _():
                w2_copy(q + n_slot_w2).start()

        @pl.when(k >= n_slot_p)
        def _():
            core_part(k - n_slot_p).wait_send()
        for s in range(n_dev):
            rhs = osum[s].astype(BF16)
            acc = jnp.dot(coef[m, 0, s], rhs, preferred_element_type=F32)
            acc += jnp.dot(coef[m, 1, s], rhs, preferred_element_type=F32)
            acc += jnp.dot(coef[m, 2, s], rhs, preferred_element_type=F32)
            part[slot, s % 2, s // 2] = acc
        core_part(k).start()

    def core_part(k):
        ps, ds = lax.rem(k, n_slot_p), lax.rem(k, n_slot_d)
        return remote(part.at[ps, other], dbuf.at[ds], d_send.at[ps], d_recv.at[ds], partner)

    def far_part(k, d):
        s = lax.rem(k, n_slot_d)
        return remote(cbuf.at[s, far_c, pl.ds(d * half, half)], rbuf.at[s, d], r_send.at[s, d], r_recv.at[s, d], side[d])

    def near_part(k, d, h):
        s, f = lax.rem(k, n_slot_d), lax.rem(k, n_slot_f)
        return remote(cbuf.at[s, (right_c, left_c)[d], pl.ds(h * half, half)], fbuf.at[f, d, pl.ds(h * half, half)],
                      f_send.at[s, d, h], f_recv.at[f, d, h], side[d])

    def y_copy(k, hbm):
        s = lax.rem(k, n_slot_d)
        col = pl.multiple_of(lax.rem(k, n_col) * CW, CW)
        return pltpu.make_async_copy(ybuf.at[s], hbm.at[:, pl.ds(col, CW)], y_sem.at[s])

    def drain_sends(k):
        for d in range(2):
            far_part(k, d).wait_send()
            near_part(k, d, 0).wait_send()
            near_part(k, d, 1).wait_send()

    def stage2(k):
        @pl.when(k >= n_slot_d)
        def _():
            drain_sends(k - n_slot_d)
        core_part(k).wait_recv()
        s = lax.rem(k, n_slot_d)
        ps = lax.rem(k, n_slot_p)
        for c in range(n_chip):
            cbuf[s, c] = part[ps, core, c] + dbuf[s, c]
        for d in range(2):
            far_part(k, d).start()
            near_part(k, d, 1 - d).start()

    def stage3(k):
        s = lax.rem(k, n_slot_d)
        for d in range(2):
            far_part(k, d).wait_recv()
            c = (right_c, left_c)[d]
            cbuf[s, c, d * half:(d + 1) * half] = cbuf[s, c, d * half:(d + 1) * half] + rbuf[s, d]
            near_part(k, d, d).start()

    def stage4(k, m, hbm):
        s, f = lax.rem(k, n_slot_d), lax.rem(k, n_slot_f)

        @pl.when(k >= n_slot_d)
        def _():
            y_copy(k - n_slot_d, hbm).wait()
        for d in range(2):
            for h in range(2):
                near_part(k, d, h).wait_recv()
        col = pl.multiple_of(lax.rem(k, n_col) * CW, CW)
        x_own = xall[m, chip, pl.ds(pl.multiple_of(core * tok, 16), tok), pl.ds(col, CW)].astype(F32)
        ybuf[s] = (x_own + (cbuf[s, chip] + fbuf[f, 0] + fbuf[f, 1])).astype(BF16)
        y_copy(k, hbm).start()

    def finish(k):
        @pl.when((k >= 1) & (k < n_step + 1))
        def _():
            stage2(k - 1)

        @pl.when((k >= 2) & (k < n_step + 2))
        def _():
            stage3(k - 2)

        @pl.when((k >= 3) & (k < n_col + 3))
        def _():
            stage4(k - 3, 0, ya_hbm)

        @pl.when(k >= n_col + 3)
        def _():
            stage4(k - 3, 1, yb_hbm)

    own_load(0).start()
    own_load(1).start()
    for t in range(n_tile):
        w1_copy(0, t).start()
    for q in range(n_slot_w2):
        w2_copy(jnp.int32(q)).start()

    barrier = pltpu.get_barrier_semaphore()
    for i in range(1, n_dev):
        pl.semaphore_signal(barrier, inc=1, device_id={'expert': lax.rem(me + i, n_dev)}, device_id_type=pl.DeviceIdType.MESH)

    for i, (ref, as_f32) in enumerate(((idx_a, True), (gate_a, False), (idx_b, True), (gate_b, False))):
        meta[me, 8 * i:8 * i + k_top] = ref[...].astype(F32) if as_f32 else ref[...]
        meta[me, 8 * i + k_top:8 * i + 8] = jnp.zeros((8 - k_top, tok), F32)
    pick_f[...] = jnp.zeros_like(pick_f)
    for s in range(n_dev):
        osum[s, n_exp * load:lanes] = jnp.zeros((lanes - n_exp * load, CW), F32)

    own_load(0).wait()
    pl.semaphore_wait(barrier, n_dev - 1)

    def meta_copy(i):
        return remote(meta.at[me], meta.at[me], meta_send.at[i], meta_recv.at[i], lax.rem(me + i, n_dev))

    def meta_arrival(i):
        src = lax.rem(me + n_dev - i, n_dev)
        return remote(meta.at[src], meta.at[src], meta_send.at[i], meta_recv.at[i], lax.rem(me + i, n_dev))

    for i in range(1, n_dev):
        meta_copy(i).start()
    start_own(0)
    for i in range(1, n_dev):
        meta_arrival(i).wait_recv()
    routing(0)
    relay_first(0)
    own_load(1).wait()
    start_own(1)
    routing(1)
    relay_second(0)
    from_partner(0, 0).wait_recv()
    gather(0, chip)
    from_partner(0, 1).wait_recv()
    gather(0, right_c)
    from_partner(0, 2).wait_recv()
    gather(0, left_c)
    relay_far(0)
    from_partner(0, 3).wait_recv()
    gather(0, far_c)

    def up_a(e, carry):
        @pl.when(e == 2)
        def _():
            relay_first(1)

        @pl.when(e == 5)
        def _():
            relay_second(1)
        up(0, e)
        return carry

    lax.fori_loop(0, n_exp, up_a, 0)

    def first_steps(k, carry):
        down(0, k)

        @pl.when(k == 0)
        def _():
            relay_far(1)
            for i in range(4):
                from_partner(1, i).wait_recv()
            for c in range(n_chip):
                gather(1, c)
        finish(k)
        up(1, k)
        return carry

    lax.fori_loop(0, n_col, first_steps, 0)

    def last_steps(k, carry):
        down(1, k)
        finish(k)
        return carry

    lax.fori_loop(n_col, n_step, last_steps, 0)

    def drain(k, carry):
        finish(k)
        return carry

    lax.fori_loop(n_step, n_step + 3, drain, 0)

    for i in range(1, n_dev):
        meta_copy(i).wait_send()
    for m in range(2):
        for d in range(2):
            for h in range(2):
                own_send(m, d, h).wait_send()
            forward(m, d).wait_send()
        for i in range(4):
            to_partner(m, i).wait_send()
    for k in range(n_step - n_slot_p, n_step):
        core_part(jnp.int32(k)).wait_send()
    for k in range(n_step - n_slot_d, n_step):
        drain_sends(jnp.int32(k))
        y_copy(jnp.int32(k), yb_hbm).wait()


def solution(mesh):
    n_dev = mesh.shape['expert']
    row_spec = P(('data', 'expert'), None)
    weight_spec = P('expert', None, None)

    def device_fn(x_a, idx_a, gate_a, x_b, idx_b, gate_b, w_up, w_down):
        tok, d_model = x_a.shape
        k_top = idx_a.shape[1]
        n_exp, _, d_ff = w_up.shape
        n_chip = n_dev // 2
        cap = tok * k_top // n_exp
        load = 2 * tok * k_top // (n_exp * n_dev)
        lanes = -(-n_exp * load // 128) * 128
        rows = n_dev * load
        half = tok // 2
        dims = (n_dev, n_chip, tok, k_top, d_model, d_ff, n_exp, load, cap)
        dma = pltpu.SemaphoreType.DMA
        any_spec = pl.BlockSpec(memory_space=pl.ANY)
        vmem_spec = pl.BlockSpec(memory_space=pltpu.VMEM)
        n_tile = -(-d_ff // TW)
        scratch = [
            pltpu.VMEM((2, n_chip, 2 * tok, d_model), BF16),
            pltpu.VMEM((n_exp, rows, d_model), BF16),
            pltpu.VMEM((2, n_exp, rows, d_ff), BF16),
            pltpu.VMEM((n_tile, d_model, TW), BF16),
            pltpu.VMEM((3, n_exp // 2, d_ff, CW), BF16),
            pltpu.VMEM((2, 3, n_dev, tok, lanes), BF16),
            pltpu.VMEM((2, n_chip, 2 * n_exp * load, 2 * tok), BF16),
            pltpu.VMEM((2 * n_exp * load, 2 * tok), F32),
            pltpu.VMEM((n_dev, 32, tok), F32),
            pltpu.VMEM((n_dev, lanes, CW), F32),
            pltpu.VMEM((2, 2, n_chip, tok, CW), F32),
            pltpu.VMEM((4, n_chip, tok, CW), F32),
            pltpu.VMEM((4, n_chip, tok, CW), F32),
            pltpu.VMEM((4, 2, half, CW), F32),
            pltpu.VMEM((8, 2, tok, CW), F32),
            pltpu.VMEM((4, tok, CW), BF16),
            dma((n_dev,)), dma((n_dev,)), dma((2,)),
            dma((2, 2, 2)), dma((2, 2, 3)), dma((2, 2)),
            dma((2, 4)), dma((2, 4)),
            dma((n_tile,)), dma((3,)),
            dma((2,)), dma((4,)),
            dma((4, 2)), dma((4, 2)),
            dma((4, 2, 2)), dma((8, 2, 2)), dma((4,)),
        ]
        return pl.pallas_call(
            functools.partial(moe_kernel, dims),
            out_shape=(jax.ShapeDtypeStruct(x_a.shape, BF16), jax.ShapeDtypeStruct(x_b.shape, BF16)),
            in_specs=[vmem_spec] * 4 + [any_spec] * 4,
            out_specs=(any_spec, any_spec),
            scratch_shapes=scratch,
            compiler_params=pltpu.CompilerParams(collective_id=0, has_side_effects=True, vmem_limit_bytes=67043328),
        )(idx_a.T, gate_a.T, idx_b.T, gate_b.T, x_a, x_b, w_up, w_down)

    return jax.shard_map(device_fn, mesh=mesh, in_specs=(row_spec, row_spec, row_spec, row_spec, row_spec, row_spec, weight_spec, weight_spec), out_specs=(row_spec, row_spec), check_vma=False)
```

```python
import functools

import jax
import jax.numpy as jnp
from jax import lax
from jax.experimental import pallas as pl
from jax.experimental.pallas import tpu as pltpu
from jax.sharding import PartitionSpec as P

F32 = jnp.float32
BF16 = jnp.bfloat16
CW = 256
TW = 512


def moe_kernel(dims, idx_a, gate_a, idx_b, gate_b, xa_hbm, xb_hbm, wu_hbm, wd_hbm, ya_ref, yb_ref,
               xall, buf, hid, w1, w2, coef, pick, pick_f, meta, osum, part, dbuf, cbuf, rbuf, fbuf,
               meta_send, meta_recv, x_sem, ag_send, ag_recv, fwd_send, core_send, core_recv,
               w1_sem, w2_sem, d_send, d_recv, r_send, r_recv, f_send, f_recv):
    n_dev, n_chip, tok, k_top, d_model, d_ff, n_exp, load, cap = dims
    lanes = coef.shape[-1]
    rows = n_dev * load
    half = tok // 2
    pair = 2 * load
    n_col = d_model // CW
    n_step = 2 * n_col
    bounds = [(t, min(TW, d_ff - t)) for t in range(0, d_ff, TW)]
    n_slot_p, n_slot_d, n_slot_c, n_slot_f = part.shape[0], dbuf.shape[0], cbuf.shape[0], fbuf.shape[0]
    n_slot_r = rbuf.shape[0]
    e_half = n_exp // 2
    n_slot_w1, n_slot_w2 = w1.shape[0], w2.shape[0]

    me = lax.axis_index('expert')
    chip, core = me // 2, lax.rem(me, 2)
    other = 1 - core
    right_c, left_c, far_c = lax.rem(chip + 1, n_chip), lax.rem(chip + n_chip - 1, n_chip), lax.rem(chip + 2, n_chip)
    partner = chip * 2 + other
    side = (right_c * 2 + core, left_c * 2 + core)

    def remote(src, dst, send, recv, dev):
        return pltpu.make_async_remote_copy(src_ref=src, dst_ref=dst, send_sem=send, recv_sem=recv,
                                            device_id={'expert': dev}, device_id_type=pl.DeviceIdType.MESH)

    def w1_copy(q):
        slot = lax.rem(q, n_slot_w1)
        return pltpu.make_async_copy(wu_hbm.at[lax.rem(q // 2, n_exp), pl.ds(lax.rem(q, 2) * (d_model // 2), d_model // 2)],
                                     w1.at[slot], w1_sem.at[slot])

    def w2_copy(q):
        step, part_id = q // 2, lax.rem(q, 2)
        col = pl.multiple_of(lax.rem(step, n_col) * CW, CW)
        slot = lax.rem(q, n_slot_w2)
        return pltpu.make_async_copy(wd_hbm.at[pl.ds(part_id * e_half, e_half), :, pl.ds(col, CW)], w2.at[slot], w2_sem.at[slot])

    def block(m, c, r0=0, n=tok, k=None):
        k = core if k is None else k
        return xall.at[m, c, pl.ds(pl.multiple_of(k * tok + r0, 16), n), :]

    def own_load(m):
        return pltpu.make_async_copy((xa_hbm, xb_hbm)[m], block(m, chip), x_sem.at[m])

    def own_send(m, d, h):
        ref = block(m, chip, h * half, half)
        return remote(ref, ref, ag_send.at[m, d, h], ag_recv.at[m, d, h], side[d])

    def own_arrival(m, d, h):
        ref = block(m, (left_c, right_c)[d], h * half, half)
        return remote(ref, ref, ag_send.at[m, d, h], ag_recv.at[m, d, h], side[d])

    def forward(m, d):
        ref = block(m, (left_c, right_c)[d], d * half, half)
        return remote(ref, ref, fwd_send.at[m, d], ag_recv.at[m, d, 2], side[d])

    def far_arrival(m, d):
        ref = block(m, far_c, d * half, half)
        return remote(ref, ref, fwd_send.at[m, d], ag_recv.at[m, d, 2], side[d])

    def to_partner(m, i):
        ref = block(m, (chip, right_c, left_c, far_c)[i])
        return remote(ref, ref, core_send.at[m, i], core_recv.at[m, i], partner)

    def from_partner(m, i):
        ref = block(m, (chip, right_c, left_c, far_c)[i], k=other)
        return remote(ref, ref, core_send.at[m, i], core_recv.at[m, i], partner)

    def relay_first(m):
        for d in range(2):
            own_arrival(m, d, d).wait_recv()
            forward(m, d).start()

    def relay_second(m):
        own_arrival(m, 1, 0).wait_recv()
        to_partner(m, 1).start()
        own_arrival(m, 0, 1).wait_recv()
        to_partner(m, 2).start()

    def relay_far(m):
        for d in range(2):
            far_arrival(m, d).wait_recv()
        to_partner(m, 3).start()

    def routing(m):
        lane = lax.broadcasted_iota(jnp.int32, (1, lanes), 1)
        lane_e = jnp.where(lane < n_exp * load, me * n_exp + lane // load, -1).astype(F32)
        lane_r = lax.rem(lane, load).astype(F32)
        row_id = lax.broadcasted_iota(jnp.int32, (tok, tok), 0)
        col_id = lax.broadcasted_iota(jnp.int32, (tok, tok), 1)
        below = jnp.where(col_id < row_id, 1.0, 0.0).astype(BF16)

        def one_source(s, before):
            facts = jnp.concatenate([meta[s], jnp.zeros((tok - meta.shape[1], tok), F32)], axis=0).T
            hit = jnp.zeros((tok, lanes), F32)
            gate = jnp.zeros((tok, lanes), F32)
            for j in range(k_top):
                same = facts[:, 16 * m + j:16 * m + j + 1] == lane_e
                hit = jnp.where(same, 1.0, hit)
                gate = jnp.where(same, facts[:, 16 * m + 8 + j:16 * m + 9 + j], gate)
            rank = jnp.dot(below, hit.astype(BF16), preferred_element_type=F32)
            keep = (hit > 0.0) & (rank == lane_r) & (before + rank < float(cap))
            gate = jnp.where(keep, gate, 0.0)
            hi = (gate * 0.9921875).astype(BF16)
            rest = gate - hi.astype(F32)
            mid = rest.astype(BF16)
            low = (rest - mid.astype(F32)).astype(BF16)
            coef[m, 0, s] = hi
            coef[m, 1, s] = mid
            coef[m, 2, s] = low
            chosen = jnp.where(keep, 1.0, 0.0).T
            return before + jnp.sum(hit, axis=0, keepdims=True), chosen

        before = jnp.zeros((1, lanes), F32)
        for c in range(n_chip):
            for k in range(2):
                before, chosen = one_source(2 * c + k, before)
                for e in range(n_exp):
                    pick_f[e * pair + k * load:e * pair + (k + 1) * load, k * tok:(k + 1) * tok] = chosen[e * load:(e + 1) * load]
            pick[m, c] = pick_f[...].astype(BF16)

    def gather(m, c):
        for n in range(0, d_model, 512):
            got = jnp.dot(pick[m, c], xall[m, c, :, n:n + 512], preferred_element_type=F32).astype(BF16)
            for e in range(n_exp):
                buf[e, pl.ds(pl.multiple_of(c * pair, 16), pair), n:n + 512] = got[e * pair:(e + 1) * pair]

    def up(m, e):
        q = 2 * (m * n_exp + e)
        depth = d_model // 2
        for h in range(2):
            w1_copy(q + h).wait()
        for lo, width in bounds:
            acc = jnp.dot(buf[e, :, 0:depth], w1[lax.rem(q, n_slot_w1), :, lo:lo + width], preferred_element_type=F32)
            acc += jnp.dot(buf[e, :, depth:], w1[lax.rem(q + 1, n_slot_w1), :, lo:lo + width], preferred_element_type=F32)
            hid[m, e, :, lo:lo + width] = jax.nn.gelu(acc, approximate=True).astype(BF16)
        for h in range(2):
            nxt = q + h + n_slot_w1

            @pl.when(nxt < 4 * n_exp)
            def _():
                w1_copy(nxt).start()

    def down(m, k):
        slot = lax.rem(k, n_slot_p)
        for p in range(2):
            w2_copy(2 * k + p).wait()

        @pl.when(k >= n_slot_p)
        def _():
            core_part(k - n_slot_p).wait_send()
        for e in range(n_exp):
            out = jnp.dot(hid[m, e], w2[lax.rem(2 * k + e // e_half, n_slot_w2), e % e_half], preferred_element_type=F32)
            for s in range(n_dev):
                osum[s, e * load:(e + 1) * load, :] = out[s * load:(s + 1) * load]
        for s in range(n_dev):
            rhs = osum[s].astype(BF16)
            acc = jnp.dot(coef[m, 0, s], rhs, preferred_element_type=F32)
            acc += jnp.dot(coef[m, 1, s], rhs, preferred_element_type=F32)
            acc += jnp.dot(coef[m, 2, s], rhs, preferred_element_type=F32)
            part[slot, s % 2, s // 2] = acc
        core_part(k).start()
        for p in range(2):
            q = 2 * k + p + n_slot_w2

            @pl.when(q < 2 * n_step)
            def _():
                w2_copy(q).start()

    def core_part(k):
        ps, ds = lax.rem(k, n_slot_p), lax.rem(k, n_slot_d)
        return remote(part.at[ps, other], dbuf.at[ds], d_send.at[ps], d_recv.at[ds], partner)

    def far_part(k, d):
        s, r = lax.rem(k, n_slot_c), lax.rem(k, n_slot_r)
        return remote(cbuf.at[s, far_c, pl.ds(d * half, half)], rbuf.at[r, d], r_send.at[s, d], r_recv.at[r, d], side[d])

    def near_part(k, d, h):
        s, f = lax.rem(k, n_slot_c), lax.rem(k, n_slot_f)
        return remote(cbuf.at[s, (right_c, left_c)[d], pl.ds(h * half, half)], fbuf.at[f, d, pl.ds(h * half, half)],
                      f_send.at[s, d, h], f_recv.at[f, d, h], side[d])

    def drain_sends(k):
        for d in range(2):
            far_part(k, d).wait_send()
            near_part(k, d, 0).wait_send()
            near_part(k, d, 1).wait_send()

    def stage2(k, late=False):
        @pl.when(k >= n_slot_c)
        def _():
            drain_sends(k - n_slot_c)
        core_part(k).wait_recv()
        s, ds, ps = lax.rem(k, n_slot_c), lax.rem(k, n_slot_d), lax.rem(k, n_slot_p)
        for c in range(n_chip):
            cbuf[s, c] = part[ps, core, c] + dbuf[ds, c]
        for d in range(2):
            far_part(k, d).start()
        if not late:
            near_halves(k)

    def near_halves(k):
        for d in range(2):
            near_part(k, d, 1 - d).start()

    def stage3(k):
        s = lax.rem(k, n_slot_c)
        for d in range(2):
            far_part(k, d).wait_recv()
            c = (right_c, left_c)[d]
            cbuf[s, c, d * half:(d + 1) * half] = cbuf[s, c, d * half:(d + 1) * half] + rbuf[lax.rem(k, n_slot_r), d]
            near_part(k, d, d).start()

    def stage4(k, m, y_ref):
        s, f = lax.rem(k, n_slot_c), lax.rem(k, n_slot_f)

        for d in range(2):
            for h in range(2):
                near_part(k, d, h).wait_recv()
        col = pl.multiple_of(lax.rem(k, n_col) * CW, CW)
        x_own = xall[m, chip, pl.ds(pl.multiple_of(core * tok, 16), tok), pl.ds(col, CW)].astype(F32)
        y_ref[:, pl.ds(col, CW)] = (x_own + (cbuf[s, chip] + fbuf[f, 0] + fbuf[f, 1])).astype(BF16)

    def stage4_at(k):
        @pl.when((k >= 0) & (k < n_col))
        def _():
            stage4(k, 0, ya_ref)

        @pl.when(k >= n_col)
        def _():
            stage4(k, 1, yb_ref)

    own_load(0).start()
    own_load(1).start()
    barrier = pltpu.get_barrier_semaphore()
    for i in range(1, n_dev):
        pl.semaphore_signal(barrier, inc=1, device_id={'expert': lax.rem(me + i, n_dev)}, device_id_type=pl.DeviceIdType.MESH)

    for i, (ref, as_f32) in enumerate(((idx_a, True), (gate_a, False), (idx_b, True), (gate_b, False))):
        meta[me, 8 * i:8 * i + k_top] = ref[...].astype(F32) if as_f32 else ref[...]
        meta[me, 8 * i + k_top:8 * i + 8] = jnp.zeros((8 - k_top, tok), F32)
    own_load(0).wait()
    own_load(1).wait()
    pl.semaphore_wait(barrier, n_dev - 1)

    def meta_copy(i):
        return remote(meta.at[me], meta.at[me], meta_send.at[i], meta_recv.at[i], lax.rem(me + i, n_dev))

    def meta_arrival(i):
        src = lax.rem(me + n_dev - i, n_dev)
        return remote(meta.at[src], meta.at[src], meta_send.at[i], meta_recv.at[i], lax.rem(me + i, n_dev))

    for i in range(1, n_dev):
        meta_copy(i).start()
    own_send(0, 0, 0).start()
    own_send(0, 1, 1).start()
    for q in range(n_slot_w1):
        w1_copy(jnp.int32(q)).start()
    for q in range(n_slot_w2):
        w2_copy(jnp.int32(q)).start()
    pick_f[...] = jnp.zeros_like(pick_f)
    for s in range(n_dev):
        osum[s, n_exp * load:lanes] = jnp.zeros((lanes - n_exp * load, CW), F32)
    to_partner(0, 0).start()
    for i in range(1, n_dev):
        meta_arrival(i).wait_recv()
    own_send(0, 0, 1).start()
    own_send(0, 1, 0).start()
    routing(0)
    relay_first(0)
    routing(1)
    relay_second(0)
    from_partner(0, 0).wait_recv()
    gather(0, chip)
    from_partner(0, 1).wait_recv()
    gather(0, right_c)
    from_partner(0, 2).wait_recv()
    gather(0, left_c)
    relay_far(0)
    own_send(1, 0, 0).start()
    own_send(1, 1, 1).start()
    to_partner(1, 0).start()
    from_partner(0, 3).wait_recv()
    gather(0, far_c)

    def up_a(e, carry):
        up(0, e)

        @pl.when(e == 0)
        def _():
            own_send(1, 0, 1).start()
            own_send(1, 1, 0).start()

        @pl.when(e == 3)
        def _():
            relay_first(1)

        @pl.when(e == 6)
        def _():
            relay_second(1)
        return carry

    lax.fori_loop(0, n_exp, up_a, 0)

    def first_steps(k, carry):
        down(0, k)

        @pl.when(k == 0)
        def _():
            for i, c in ((0, chip), (1, right_c)):
                from_partner(1, i).wait_recv()
                gather(1, c)
            stage2(k)
            relay_far(1)

        @pl.when(k == 1)
        def _():
            for i, c in ((2, left_c), (3, far_c)):
                from_partner(1, i).wait_recv()
                gather(1, c)

        @pl.when(k >= 2)
        def _():
            up(1, k - 2)
        stage4_at(k - 3)

        @pl.when(k >= 1)
        def _():
            stage2(k)
            stage3(k - 1)
        return carry

    lax.fori_loop(0, n_col, first_steps, 0)

    def rest_up(e, carry):
        up(1, e)
        return carry

    lax.fori_loop(n_col - 2, n_exp, rest_up, 0)

    def last_steps(k, carry):
        down(1, k)
        stage4_at(k - 3)
        stage2(k)
        stage3(k - 1)
        return carry

    lax.fori_loop(n_col, n_step - 1, last_steps, 0)
    last = jnp.int32(n_step - 1)
    down(1, last)
    stage4(last - 3, 1, yb_ref)
    stage2(last, late=True)
    stage3(last - 1)
    near_halves(last)
    stage4(last - 2, 1, yb_ref)
    stage3(last)
    stage4(last - 1, 1, yb_ref)
    stage4(last, 1, yb_ref)

    for i in range(1, n_dev):
        meta_copy(i).wait_send()
    for m in range(2):
        for d in range(2):
            for h in range(2):
                own_send(m, d, h).wait_send()
            forward(m, d).wait_send()
        for i in range(4):
            to_partner(m, i).wait_send()
    for k in range(n_step - n_slot_p, n_step):
        core_part(jnp.int32(k)).wait_send()
    for k in range(n_step - n_slot_c, n_step):
        drain_sends(jnp.int32(k))


def solution(mesh):
    n_dev = mesh.shape['expert']
    row_spec = P(('data', 'expert'), None)
    weight_spec = P('expert', None, None)

    def device_fn(x_a, idx_a, gate_a, x_b, idx_b, gate_b, w_up, w_down):
        tok, d_model = x_a.shape
        k_top = idx_a.shape[1]
        n_exp, _, d_ff = w_up.shape
        n_chip = n_dev // 2
        cap = tok * k_top // n_exp
        load = 2 * tok * k_top // (n_exp * n_dev)
        lanes = -(-n_exp * load // 128) * 128
        rows = n_dev * load
        half = tok // 2
        dims = (n_dev, n_chip, tok, k_top, d_model, d_ff, n_exp, load, cap)
        dma = pltpu.SemaphoreType.DMA
        any_spec = pl.BlockSpec(memory_space=pl.ANY)
        vmem_spec = pl.BlockSpec(memory_space=pltpu.VMEM)
        scratch = [
            pltpu.VMEM((2, n_chip, 2 * tok, d_model), BF16),
            pltpu.VMEM((n_exp, rows, d_model), BF16),
            pltpu.VMEM((2, n_exp, rows, d_ff), BF16),
            pltpu.VMEM((5, d_model // 2, d_ff), BF16),
            pltpu.VMEM((3, n_exp // 2, d_ff, CW), BF16),
            pltpu.VMEM((2, 3, n_dev, tok, lanes), BF16),
            pltpu.VMEM((2, n_chip, 2 * n_exp * load, 2 * tok), BF16),
            pltpu.VMEM((2 * n_exp * load, 2 * tok), F32),
            pltpu.VMEM((n_dev, 32, tok), F32),
            pltpu.VMEM((n_dev, lanes, CW), F32),
            pltpu.VMEM((2, 2, n_chip, tok, CW), F32),
            pltpu.VMEM((2, n_chip, tok, CW), F32),
            pltpu.VMEM((3, n_chip, tok, CW), F32),
            pltpu.VMEM((4, 2, half, CW), F32),
            pltpu.VMEM((5, 2, tok, CW), F32),
            dma((n_dev,)), dma((n_dev,)), dma((2,)),
            dma((2, 2, 2)), dma((2, 2, 3)), dma((2, 2)),
            dma((2, 4)), dma((2, 4)),
            dma((5,)), dma((3,)),
            dma((2,)), dma((2,)),
            dma((3, 2)), dma((4, 2)),
            dma((3, 2, 2)), dma((5, 2, 2)),
        ]
        return pl.pallas_call(
            functools.partial(moe_kernel, dims),
            out_shape=(pltpu.VMEM(x_a.shape, BF16), pltpu.VMEM(x_b.shape, BF16)),
            in_specs=[vmem_spec] * 4 + [any_spec] * 4,
            out_specs=(vmem_spec, vmem_spec),
            scratch_shapes=scratch,
            compiler_params=pltpu.CompilerParams(collective_id=0, has_side_effects=True, vmem_limit_bytes=65994752),
        )(idx_a.T, gate_a.T, idx_b.T, gate_b.T, x_a, x_b, w_up, w_down)

    return jax.shard_map(device_fn, mesh=mesh, in_specs=(row_spec, row_spec, row_spec, row_spec, row_spec, row_spec, weight_spec, weight_spec), out_specs=(row_spec, row_spec), check_vma=False)
```

```python
import functools

import jax
import jax.numpy as jnp
from jax import lax
from jax.experimental import pallas as pl
from jax.experimental.pallas import tpu as pltpu
from jax.sharding import PartitionSpec as P

F32 = jnp.float32
BF16 = jnp.bfloat16
CW = 256
TW = 512


def moe_kernel(dims, idx_a_hbm, gate_a_hbm, idx_b_hbm, gate_b_hbm, xa_hbm, xb_hbm, wu_hbm, wd_hbm, ya_ref, yb_ref,
               xall, buf, hid, w1, w2, coef, pick, pick_f, idx_v, gate_v, meta, osum, part, dbuf, cbuf, rbuf, fbuf,
               meta_send, meta_recv, route_sem, x_sem, ag_send, ag_recv, fwd_send, core_send, core_recv,
               w1_sem, w2_sem, d_send, d_recv, r_send, r_recv, f_send, f_recv):
    n_dev, n_chip, tok, k_top, d_model, d_ff, n_exp, load, cap = dims
    lanes = coef.shape[-1]
    rows = n_dev * load
    half = tok // 2
    pair = 2 * load
    n_col = d_model // CW
    n_step = 2 * n_col
    bounds = [(t, min(TW, d_ff - t)) for t in range(0, d_ff, TW)]
    n_slot_p, n_slot_d, n_slot_c, n_slot_f = part.shape[0], dbuf.shape[0], cbuf.shape[0], fbuf.shape[0]
    n_slot_r = rbuf.shape[0]
    e_half = n_exp // 2
    n_slot_w1, n_slot_w2 = w1.shape[0], w2.shape[0]

    me = lax.axis_index('expert')
    chip, core = me // 2, lax.rem(me, 2)
    other = 1 - core
    right_c, left_c, far_c = lax.rem(chip + 1, n_chip), lax.rem(chip + n_chip - 1, n_chip), lax.rem(chip + 2, n_chip)
    partner = chip * 2 + other
    side = (right_c * 2 + core, left_c * 2 + core)

    def remote(src, dst, send, recv, dev):
        return pltpu.make_async_remote_copy(src_ref=src, dst_ref=dst, send_sem=send, recv_sem=recv,
                                            device_id={'expert': dev}, device_id_type=pl.DeviceIdType.MESH)

    def w1_copy(q):
        slot = lax.rem(q, n_slot_w1)
        return pltpu.make_async_copy(wu_hbm.at[lax.rem(q // 2, n_exp), pl.ds(lax.rem(q, 2) * (d_model // 2), d_model // 2)],
                                     w1.at[slot], w1_sem.at[slot])

    def w2_copy(q):
        step, part_id = q // 2, lax.rem(q, 2)
        col = pl.multiple_of(lax.rem(step, n_col) * CW, CW)
        slot = lax.rem(q, n_slot_w2)
        return pltpu.make_async_copy(wd_hbm.at[pl.ds(part_id * e_half, e_half), :, pl.ds(col, CW)], w2.at[slot], w2_sem.at[slot])

    def block(m, c, r0=0, n=tok, k=None):
        k = core if k is None else k
        return xall.at[m, c, pl.ds(pl.multiple_of(k * tok + r0, 16), n), :]

    def own_load(m):
        return pltpu.make_async_copy((xa_hbm, xb_hbm)[m], block(m, chip), x_sem.at[m])

    def own_send(m, d, h):
        ref = block(m, chip, h * half, half)
        return remote(ref, ref, ag_send.at[m, d, h], ag_recv.at[m, d, h], side[d])

    def own_arrival(m, d, h):
        ref = block(m, (left_c, right_c)[d], h * half, half)
        return remote(ref, ref, ag_send.at[m, d, h], ag_recv.at[m, d, h], side[d])

    def forward(m, d):
        ref = block(m, (left_c, right_c)[d], d * half, half)
        return remote(ref, ref, fwd_send.at[m, d], ag_recv.at[m, d, 2], side[d])

    def far_arrival(m, d):
        ref = block(m, far_c, d * half, half)
        return remote(ref, ref, fwd_send.at[m, d], ag_recv.at[m, d, 2], side[d])

    def to_partner(m, i):
        ref = block(m, (chip, right_c, left_c, far_c)[i])
        return remote(ref, ref, core_send.at[m, i], core_recv.at[m, i], partner)

    def far_to_partner(m, d, k):
        ref = block(m, far_c, d * half, half, k=k)
        return remote(ref, ref, core_send.at[m, 3 + d], core_recv.at[m, 3 + d], partner)

    def far_from_partner(m):
        for d in range(2):
            far_to_partner(m, d, other).wait_recv()

    def from_partner(m, i):
        ref = block(m, (chip, right_c, left_c, far_c)[i], k=other)
        return remote(ref, ref, core_send.at[m, i], core_recv.at[m, i], partner)

    def relay_first(m):
        for d in range(2):
            own_arrival(m, d, d).wait_recv()
            forward(m, d).start()

    def relay_second(m):
        own_arrival(m, 1, 0).wait_recv()
        to_partner(m, 1).start()
        own_arrival(m, 0, 1).wait_recv()
        to_partner(m, 2).start()

    def relay_far(m):
        for d in range(2):
            far_arrival(m, d).wait_recv()
            far_to_partner(m, d, core).start()

    def routing(m, between=()):
        lane = lax.broadcasted_iota(jnp.int32, (1, lanes), 1)
        lane_e = jnp.where(lane < n_exp * load, me * n_exp + lane // load, -1).astype(F32)
        lane_r = lax.rem(lane, load).astype(F32)
        row_id = lax.broadcasted_iota(jnp.int32, (tok, tok), 0)
        col_id = lax.broadcasted_iota(jnp.int32, (tok, tok), 1)
        below = jnp.where(col_id < row_id, 1.0, 0.0).astype(BF16)

        def one_source(s, before):
            facts = jnp.concatenate([meta[m, s], jnp.zeros((tok - meta.shape[2], tok), F32)], axis=0).T
            hit = jnp.zeros((tok, lanes), F32)
            gate = jnp.zeros((tok, lanes), F32)
            for j in range(k_top):
                same = facts[:, j:j + 1] == lane_e
                hit = jnp.where(same, 1.0, hit)
                gate = jnp.where(same, facts[:, 8 + j:9 + j], gate)
            rank = jnp.dot(below, hit.astype(BF16), preferred_element_type=F32)
            keep = (hit > 0.0) & (rank == lane_r) & (before + rank < float(cap))
            gate = jnp.where(keep, gate, 0.0)
            hi = (gate * 0.9921875).astype(BF16)
            rest = gate - hi.astype(F32)
            mid = rest.astype(BF16)
            low = (rest - mid.astype(F32)).astype(BF16)
            coef[m, 0, s] = hi
            coef[m, 1, s] = mid
            coef[m, 2, s] = low
            chosen = jnp.where(keep, 1.0, 0.0).T
            return before + jnp.sum(hit, axis=0, keepdims=True), chosen

        before = jnp.zeros((1, lanes), F32)
        for c in range(n_chip):
            for k in range(2):
                before, chosen = one_source(2 * c + k, before)
                for e in range(n_exp):
                    pick_f[e * pair + k * load:e * pair + (k + 1) * load, k * tok:(k + 1) * tok] = chosen[e * load:(e + 1) * load]
            pick[m, c] = pick_f[...].astype(BF16)
            if c < len(between):
                between[c]()

    def gather(m, c):
        for n in range(0, d_model, 512):
            got = jnp.dot(pick[m, c], xall[m, c, :, n:n + 512], preferred_element_type=F32).astype(BF16)
            for e in range(n_exp):
                buf[e, pl.ds(pl.multiple_of(c * pair, 16), pair), n:n + 512] = got[e * pair:(e + 1) * pair]

    def up_wait(m, e):
        for h in range(2):
            w1_copy(2 * (m * n_exp + e) + h).wait()

    def up_math(m, e):
        q = 2 * (m * n_exp + e)
        depth = d_model // 2
        for lo, width in bounds:
            acc = jnp.dot(buf[e, :, 0:depth], w1[lax.rem(q, n_slot_w1), :, lo:lo + width], preferred_element_type=F32)
            acc += jnp.dot(buf[e, :, depth:], w1[lax.rem(q + 1, n_slot_w1), :, lo:lo + width], preferred_element_type=F32)
            hid[m, e, :, lo:lo + width] = jax.nn.gelu(acc, approximate=True).astype(BF16)

    def up_next(m, e):
        for h in range(2):
            nxt = 2 * (m * n_exp + e) + h + n_slot_w1

            @pl.when(nxt < 4 * n_exp)
            def _():
                w1_copy(nxt).start()

    def up(m, e):
        up_wait(m, e)
        up_math(m, e)
        up_next(m, e)

    def down_wait(k):
        for p in range(2):
            w2_copy(2 * k + p).wait()

        @pl.when(k >= n_slot_p)
        def _():
            core_part(k - n_slot_p).wait_send()

    def down_math(m, k):
        slot = lax.rem(k, n_slot_p)
        for e in range(n_exp):
            out = jnp.dot(hid[m, e], w2[lax.rem(2 * k + e // e_half, n_slot_w2), e % e_half], preferred_element_type=F32)
            for s in range(n_dev):
                osum[s, e * load:(e + 1) * load, :] = out[s * load:(s + 1) * load]
        for s in range(n_dev):
            rhs = osum[s].astype(BF16)
            acc = jnp.dot(coef[m, 0, s], rhs, preferred_element_type=F32)
            acc += jnp.dot(coef[m, 1, s], rhs, preferred_element_type=F32)
            acc += jnp.dot(coef[m, 2, s], rhs, preferred_element_type=F32)
            part[slot, s % 2, s // 2] = acc
        core_part(k).start()

    def down_next(k):
        for p in range(2):
            q = 2 * k + p + n_slot_w2

            @pl.when(q < 2 * n_step)
            def _():
                w2_copy(q).start()

    def down(m, k):
        down_wait(k)
        down_math(m, k)
        down_next(k)

    def core_part(k):
        ps, ds = lax.rem(k, n_slot_p), lax.rem(k, n_slot_d)
        return remote(part.at[ps, other], dbuf.at[ds], d_send.at[ps], d_recv.at[ds], partner)

    def far_part(k, d):
        s, r = lax.rem(k, n_slot_c), lax.rem(k, n_slot_r)
        return remote(cbuf.at[s, far_c, pl.ds(d * half, half)], rbuf.at[r, d], r_send.at[s, d], r_recv.at[r, d], side[d])

    def near_part(k, d, h):
        s, f = lax.rem(k, n_slot_c), lax.rem(k, n_slot_f)
        return remote(cbuf.at[s, (right_c, left_c)[d], pl.ds(h * half, half)], fbuf.at[f, d, pl.ds(h * half, half)],
                      f_send.at[s, d, h], f_recv.at[f, d, h], side[d])

    def drain_sends(k, relays=True):
        for d in range(2):
            if relays:
                far_part(k, d).wait_send()
            near_part(k, d, 0).wait_send()
            near_part(k, d, 1).wait_send()

    def stage2(k, late=False):
        @pl.when(k >= n_slot_c)
        def _():
            drain_sends(k - n_slot_c)
        core_part(k).wait_recv()
        s, ds, ps = lax.rem(k, n_slot_c), lax.rem(k, n_slot_d), lax.rem(k, n_slot_p)
        for c in range(n_chip):
            cbuf[s, c] = part[ps, core, c] + dbuf[ds, c]
        for d in range(2):
            far_part(k, d).start()
        if not late:
            near_halves(k)

    def near_halves(k):
        for d in range(2):
            near_part(k, d, 1 - d).start()

    def stage3(k):
        s = lax.rem(k, n_slot_c)
        for d in range(2):
            far_part(k, d).wait_recv()
            c = (right_c, left_c)[d]
            cbuf[s, c, d * half:(d + 1) * half] = cbuf[s, c, d * half:(d + 1) * half] + rbuf[lax.rem(k, n_slot_r), d]
            near_part(k, d, d).start()

    def stage4(k, m, y_ref):
        s, f = lax.rem(k, n_slot_c), lax.rem(k, n_slot_f)

        for d in range(2):
            for h in range(2):
                near_part(k, d, h).wait_recv()
        col = pl.multiple_of(lax.rem(k, n_col) * CW, CW)
        x_own = xall[m, chip, pl.ds(pl.multiple_of(core * tok, 16), tok), pl.ds(col, CW)].astype(F32)
        y_ref[:, pl.ds(col, CW)] = (x_own + (cbuf[s, chip] + fbuf[f, 0] + fbuf[f, 1])).astype(BF16)

    def stage4_at(k):
        @pl.when((k >= 0) & (k < n_col))
        def _():
            stage4(k, 0, ya_ref)

        @pl.when(k >= n_col)
        def _():
            stage4(k, 1, yb_ref)

    barrier = pltpu.get_barrier_semaphore()
    for i in range(1, n_dev):
        pl.semaphore_signal(barrier, inc=1, device_id={'expert': lax.rem(me + i, n_dev)}, device_id_type=pl.DeviceIdType.MESH)
    own_load(0).start()
    route_loads = [pltpu.make_async_copy(src, dst, route_sem.at[i]) for i, (src, dst) in enumerate(
        ((idx_a_hbm, idx_v.at[0]), (gate_a_hbm, gate_v.at[0]), (idx_b_hbm, idx_v.at[1]), (gate_b_hbm, gate_v.at[1])))]
    for copy in route_loads:
        copy.start()
    own_load(1).start()
    for copy in route_loads:
        copy.wait()
    for m in range(2):
        meta[m, me, 0:k_top] = idx_v[m].astype(F32)
        meta[m, me, k_top:8] = jnp.zeros((8 - k_top, tok), F32)
        meta[m, me, 8:8 + k_top] = gate_v[m]
        meta[m, me, 8 + k_top:16] = jnp.zeros((8 - k_top, tok), F32)
    own_load(0).wait()
    pl.semaphore_wait(barrier, n_dev - 1)

    right, left = side
    far = far_c * 2 + core

    def meta_copy(m, dev, i, to):
        return remote(meta.at[m, dev], meta.at[m, dev], meta_send.at[m, i], meta_recv.at[m, i], to)

    def meta_sends(m):
        return [meta_copy(m, me, 0, right), meta_copy(m, me, 1, left), meta_copy(m, me, 2, far), meta_copy(m, me, 3, partner),
                meta_copy(m, left, 4, partner), meta_copy(m, right, 5, partner), meta_copy(m, far, 6, partner)]

    def meta_arrivals(m):
        return [meta_copy(m, left, 0, right), meta_copy(m, right, 1, left), meta_copy(m, far, 2, far)] + [
            meta_copy(m, c * 2 + other, 3 + i, partner) for i, c in enumerate((chip, left_c, right_c, far_c))]

    def meta_start(m):
        for copy in meta_sends(m)[:4]:
            copy.start()

    def meta_share(m):
        for i in range(3):
            meta_arrivals(m)[i].wait_recv()
            meta_sends(m)[4 + i].start()

    def meta_end(m):
        for copy in meta_arrivals(m)[3:]:
            copy.wait_recv()

    meta_start(0)
    own_send(0, 0, 0).start()
    own_send(0, 1, 1).start()
    meta_start(1)
    own_send(0, 0, 1).start()
    own_send(0, 1, 0).start()
    for q in range(n_slot_w1):
        w1_copy(jnp.int32(q)).start()
    for q in range(n_slot_w2):
        w2_copy(jnp.int32(q)).start()
    pick_f[...] = jnp.zeros_like(pick_f)
    for s in range(n_dev):
        osum[s, n_exp * load:lanes] = jnp.zeros((lanes - n_exp * load, CW), F32)
    to_partner(0, 0).start()
    meta_share(0)
    meta_end(0)
    routing(0, (lambda: None, lambda: None, lambda: None, lambda: relay_first(0)))
    meta_share(1)
    own_load(1).wait()
    meta_end(1)
    routing(1)
    from_partner(0, 0).wait_recv()
    gather(0, chip)
    relay_second(0)
    from_partner(0, 1).wait_recv()
    gather(0, right_c)
    from_partner(0, 2).wait_recv()
    gather(0, left_c)
    relay_far(0)
    own_send(1, 0, 0).start()
    own_send(1, 1, 1).start()
    to_partner(1, 0).start()
    far_from_partner(0)
    gather(0, far_c)

    def up_a(e, carry):
        up(0, e)

        @pl.when(e == 0)
        def _():
            own_send(1, 0, 1).start()
            own_send(1, 1, 0).start()

        @pl.when(e == 4)
        def _():
            relay_first(1)

        @pl.when(e == n_exp - 1)
        def _():
            relay_second(1)
        return carry

    lax.fori_loop(0, n_exp, up_a, 0)

    down(0, jnp.int32(0))
    from_partner(1, 0).wait_recv()
    gather(1, chip)
    stage2(jnp.int32(0))
    relay_far(1)
    down(0, jnp.int32(1))
    for i, c in ((1, right_c), (2, left_c)):
        from_partner(1, i).wait_recv()
        gather(1, c)
    far_from_partner(1)
    gather(1, far_c)
    stage2(jnp.int32(1))
    stage3(jnp.int32(0))

    def first_steps(k, carry):
        down(0, k)
        up(1, k - 2)
        stage4_at(k - 3)
        stage2(k)
        stage3(k - 1)
        return carry

    lax.fori_loop(2, n_col, first_steps, 0)

    def rest_up(e, carry):
        up(1, e)
        return carry

    lax.fori_loop(n_col - 2, n_exp, rest_up, 0)

    def last_steps(k, carry):
        down(1, k)
        stage4_at(k - 3)
        stage2(k)
        stage3(k - 1)
        return carry

    lax.fori_loop(n_col, n_step, last_steps, 0)
    last = jnp.int32(n_step - 1)
    stage4(last - 2, 1, yb_ref)
    stage3(last)
    stage4(last - 1, 1, yb_ref)
    stage4(last, 1, yb_ref)

    for m in range(2):
        for copy in meta_sends(m):
            copy.wait_send()
    for m in range(2):
        for d in range(2):
            for h in range(2):
                own_send(m, d, h).wait_send()
            forward(m, d).wait_send()
        for i in range(3):
            to_partner(m, i).wait_send()
        for d in range(2):
            far_to_partner(m, d, core).wait_send()
    for k in range(n_step - n_slot_p, n_step):
        core_part(jnp.int32(k)).wait_send()
    for k in range(n_step - n_slot_c, n_step):
        drain_sends(jnp.int32(k))


def write_out(ya_vmem, yb_vmem, ya_hbm, yb_hbm, sem):
    copies = [pltpu.make_async_copy(src, dst, sem.at[i]) for i, (src, dst) in enumerate(((ya_vmem, ya_hbm), (yb_vmem, yb_hbm)))]
    for copy in copies:
        copy.start()
    for copy in copies:
        copy.wait()


def solution(mesh):
    n_dev = mesh.shape['expert']
    row_spec = P(('data', 'expert'), None)
    weight_spec = P('expert', None, None)

    def device_fn(x_a, idx_a, gate_a, x_b, idx_b, gate_b, w_up, w_down):
        tok, d_model = x_a.shape
        k_top = idx_a.shape[1]
        n_exp, _, d_ff = w_up.shape
        n_chip = n_dev // 2
        cap = tok * k_top // n_exp
        load = 2 * tok * k_top // (n_exp * n_dev)
        lanes = -(-n_exp * load // 128) * 128
        rows = n_dev * load
        half = tok // 2
        dims = (n_dev, n_chip, tok, k_top, d_model, d_ff, n_exp, load, cap)
        dma = pltpu.SemaphoreType.DMA
        any_spec = pl.BlockSpec(memory_space=pl.ANY)
        vmem_spec = pl.BlockSpec(memory_space=pltpu.VMEM)
        scratch = [
            pltpu.VMEM((2, n_chip, 2 * tok, d_model), BF16),
            pltpu.VMEM((n_exp, rows, d_model), BF16),
            pltpu.VMEM((2, n_exp, rows, d_ff), BF16),
            pltpu.VMEM((5, d_model // 2, d_ff), BF16),
            pltpu.VMEM((3, n_exp // 2, d_ff, CW), BF16),
            pltpu.VMEM((2, 3, n_dev, tok, lanes), BF16),
            pltpu.VMEM((2, n_chip, 2 * n_exp * load, 2 * tok), BF16),
            pltpu.VMEM((2 * n_exp * load, 2 * tok), F32),
            pltpu.VMEM((2, k_top, tok), jnp.int32),
            pltpu.VMEM((2, k_top, tok), F32),
            pltpu.VMEM((2, n_dev, 16, tok), F32),
            pltpu.VMEM((n_dev, lanes, CW), F32),
            pltpu.VMEM((2, 2, n_chip, tok, CW), F32),
            pltpu.VMEM((2, n_chip, tok, CW), F32),
            pltpu.VMEM((3, n_chip, tok, CW), F32),
            pltpu.VMEM((4, 2, half, CW), F32),
            pltpu.VMEM((5, 2, tok, CW), F32),
            dma((2, 7)), dma((2, 7)), dma((4,)), dma((2,)),
            dma((2, 2, 2)), dma((2, 2, 3)), dma((2, 2)),
            dma((2, 5)), dma((2, 5)),
            dma((5,)), dma((3,)),
            dma((2,)), dma((2,)),
            dma((3, 2)), dma((4, 2)),
            dma((3, 2, 2)), dma((5, 2, 2)),
        ]
        y_a, y_b = pl.pallas_call(
            functools.partial(moe_kernel, dims),
            out_shape=(pltpu.VMEM(x_a.shape, BF16), pltpu.VMEM(x_b.shape, BF16)),
            in_specs=[any_spec] * 8,
            out_specs=(vmem_spec, vmem_spec),
            scratch_shapes=scratch,
            compiler_params=pltpu.CompilerParams(collective_id=0, has_side_effects=True, vmem_limit_bytes=65994752),
        )(idx_a.T, gate_a.T, idx_b.T, gate_b.T, x_a, x_b, w_up, w_down)
        return pl.pallas_call(
            write_out,
            out_shape=(jax.ShapeDtypeStruct(x_a.shape, BF16), jax.ShapeDtypeStruct(x_b.shape, BF16)),
            in_specs=[vmem_spec] * 2,
            out_specs=(any_spec, any_spec),
            scratch_shapes=[dma((2,))],
        )(pltpu.with_memory_space_constraint(y_a, pltpu.VMEM), pltpu.with_memory_space_constraint(y_b, pltpu.VMEM))

    return jax.shard_map(device_fn, mesh=mesh, in_specs=(row_spec, row_spec, row_spec, row_spec, row_spec, row_spec, weight_spec, weight_spec), out_specs=(row_spec, row_spec), check_vma=False)
```

```python
import functools

import jax
import jax.numpy as jnp
from jax import lax
from jax.experimental import pallas as pl
from jax.experimental.pallas import tpu as pltpu
from jax.sharding import PartitionSpec as P

F32 = jnp.float32
BF16 = jnp.bfloat16
CW = 256
TW = 512


def moe_kernel(dims, idx_a_hbm, gate_a_hbm, idx_b_hbm, gate_b_hbm, xa_hbm, xb_hbm, wu_hbm, wd_hbm, ya_ref, yb_ref,
               xall, buf, hid, w1, w2, coef, pick, pick_f, idx_v, gate_v, meta, osum, part, dbuf, cbuf, rbuf, fbuf,
               meta_send, meta_recv, route_sem, x_sem, ag_send, ag_recv, fwd_send, core_send, core_recv,
               w1_sem, w2_sem, d_send, d_recv, r_send, r_recv, f_send, f_recv):
    n_dev, n_chip, tok, k_top, d_model, d_ff, n_exp, load, cap = dims
    lanes = coef.shape[-1]
    rows = n_dev * load
    half = tok // 2
    pair = 2 * load
    n_col = d_model // CW
    n_step = 2 * n_col
    bounds = [(t, min(TW, d_ff - t)) for t in range(0, d_ff, TW)]
    n_slot_p, n_slot_d, n_slot_c, n_slot_f = part.shape[0], dbuf.shape[0], cbuf.shape[0], fbuf.shape[0]
    n_slot_r = rbuf.shape[0]
    e_half = n_exp // 2
    n_slot_w1, n_slot_w2 = w1.shape[0], w2.shape[0]

    me = lax.axis_index('expert')
    chip, core = me // 2, lax.rem(me, 2)
    other = 1 - core
    right_c, left_c, far_c = lax.rem(chip + 1, n_chip), lax.rem(chip + n_chip - 1, n_chip), lax.rem(chip + 2, n_chip)
    partner = chip * 2 + other
    side = (right_c * 2 + core, left_c * 2 + core)

    def remote(src, dst, send, recv, dev):
        return pltpu.make_async_remote_copy(src_ref=src, dst_ref=dst, send_sem=send, recv_sem=recv,
                                            device_id={'expert': dev}, device_id_type=pl.DeviceIdType.MESH)

    def w1_copy(q):
        slot = lax.rem(q, n_slot_w1)
        return pltpu.make_async_copy(wu_hbm.at[lax.rem(q // 2, n_exp), pl.ds(lax.rem(q, 2) * (d_model // 2), d_model // 2)],
                                     w1.at[slot], w1_sem.at[slot])

    def w2_copy(q):
        step, part_id = q // 2, lax.rem(q, 2)
        col = pl.multiple_of(lax.rem(step, n_col) * CW, CW)
        slot = lax.rem(q, n_slot_w2)
        return pltpu.make_async_copy(wd_hbm.at[pl.ds(part_id * e_half, e_half), :, pl.ds(col, CW)], w2.at[slot], w2_sem.at[slot])

    def block(m, c, r0=0, n=tok, k=None):
        k = core if k is None else k
        return xall.at[m, c, pl.ds(pl.multiple_of(k * tok + r0, 16), n), :]

    def own_load(m):
        return pltpu.make_async_copy((xa_hbm, xb_hbm)[m], block(m, chip), x_sem.at[m])

    def own_send(m, d, h):
        ref = block(m, chip, h * half, half)
        return remote(ref, ref, ag_send.at[m, d, h], ag_recv.at[m, d, h], side[d])

    def own_arrival(m, d, h):
        ref = block(m, (left_c, right_c)[d], h * half, half)
        return remote(ref, ref, ag_send.at[m, d, h], ag_recv.at[m, d, h], side[d])

    def forward(m, d):
        ref = block(m, (left_c, right_c)[d], d * half, half)
        return remote(ref, ref, fwd_send.at[m, d], ag_recv.at[m, d, 2], side[d])

    def far_arrival(m, d):
        ref = block(m, far_c, d * half, half)
        return remote(ref, ref, fwd_send.at[m, d], ag_recv.at[m, d, 2], side[d])

    def to_partner(m, i):
        ref = block(m, (chip, right_c, left_c, far_c)[i])
        return remote(ref, ref, core_send.at[m, i], core_recv.at[m, i], partner)

    def far_to_partner(m, d, k):
        ref = block(m, far_c, d * half, half, k=k)
        return remote(ref, ref, core_send.at[m, 3 + d], core_recv.at[m, 3 + d], partner)

    def far_from_partner(m):
        for d in range(2):
            far_to_partner(m, d, other).wait_recv()

    def from_partner(m, i):
        ref = block(m, (chip, right_c, left_c, far_c)[i], k=other)
        return remote(ref, ref, core_send.at[m, i], core_recv.at[m, i], partner)

    def relay_first(m):
        for d in range(2):
            own_arrival(m, d, d).wait_recv()
            forward(m, d).start()

    def relay_second(m):
        own_arrival(m, 1, 0).wait_recv()
        to_partner(m, 1).start()
        own_arrival(m, 0, 1).wait_recv()
        to_partner(m, 2).start()

    def relay_far(m):
        for d in range(2):
            far_arrival(m, d).wait_recv()
            far_to_partner(m, d, core).start()

    def routing(m):
        lane = lax.broadcasted_iota(jnp.int32, (1, lanes), 1)
        lane_e = jnp.where(lane < n_exp * load, me * n_exp + lane // load, -1).astype(F32)
        lane_r = lax.rem(lane, load).astype(F32)
        row_id = lax.broadcasted_iota(jnp.int32, (tok, tok), 0)
        col_id = lax.broadcasted_iota(jnp.int32, (tok, tok), 1)
        below = jnp.where(col_id < row_id, 1.0, 0.0).astype(BF16)

        def one_source(s, before):
            facts = jnp.concatenate([meta[m, s], jnp.zeros((tok - meta.shape[2], tok), F32)], axis=0).T
            hit = jnp.zeros((tok, lanes), F32)
            gate = jnp.zeros((tok, lanes), F32)
            for j in range(k_top):
                same = facts[:, j:j + 1] == lane_e
                hit = jnp.where(same, 1.0, hit)
                gate = jnp.where(same, facts[:, 8 + j:9 + j], gate)
            rank = jnp.dot(below, hit.astype(BF16), preferred_element_type=F32)
            keep = (hit > 0.0) & (rank == lane_r) & (before + rank < float(cap))
            gate = jnp.where(keep, gate, 0.0)
            hi = (gate * 0.9921875).astype(BF16)
            rest = gate - hi.astype(F32)
            mid = rest.astype(BF16)
            low = (rest - mid.astype(F32)).astype(BF16)
            coef[m, 0, s] = hi
            coef[m, 1, s] = mid
            coef[m, 2, s] = low
            chosen = jnp.where(keep, 1.0, 0.0).T
            return before + jnp.sum(hit, axis=0, keepdims=True), chosen

        before = jnp.zeros((1, lanes), F32)
        for c in range(n_chip):
            for k in range(2):
                before, chosen = one_source(2 * c + k, before)
                for e in range(n_exp):
                    pick_f[e * pair + k * load:e * pair + (k + 1) * load, k * tok:(k + 1) * tok] = chosen[e * load:(e + 1) * load]
            pick[m, c] = pick_f[...].astype(BF16)

    def gather(m, c):
        for n in range(0, d_model, 512):
            got = jnp.dot(pick[m, c], xall[m, c, :, n:n + 512], preferred_element_type=F32).astype(BF16)
            for e in range(n_exp):
                buf[e, pl.ds(pl.multiple_of(c * pair, 16), pair), n:n + 512] = got[e * pair:(e + 1) * pair]

    def up_wait(m, e):
        for h in range(2):
            w1_copy(2 * (m * n_exp + e) + h).wait()

    def up_math(m, e):
        q = 2 * (m * n_exp + e)
        depth = d_model // 2
        for lo, width in bounds:
            acc = jnp.dot(buf[e, :, 0:depth], w1[lax.rem(q, n_slot_w1), :, lo:lo + width], preferred_element_type=F32)
            acc += jnp.dot(buf[e, :, depth:], w1[lax.rem(q + 1, n_slot_w1), :, lo:lo + width], preferred_element_type=F32)
            hid[m, e, :, lo:lo + width] = jax.nn.gelu(acc, approximate=True).astype(BF16)

    def up_next(m, e):
        for h in range(2):
            nxt = 2 * (m * n_exp + e) + h + n_slot_w1

            @pl.when(nxt < 4 * n_exp)
            def _():
                w1_copy(nxt).start()

    def up(m, e):
        up_wait(m, e)
        up_math(m, e)
        up_next(m, e)

    def down_wait(k):
        for p in range(2):
            w2_copy(2 * k + p).wait()

        @pl.when(k >= n_slot_p)
        def _():
            core_part(k - n_slot_p).wait_send()

    def down_math(m, k):
        slot = lax.rem(k, n_slot_p)
        for e in range(n_exp):
            out = jnp.dot(hid[m, e], w2[lax.rem(2 * k + e // e_half, n_slot_w2), e % e_half], preferred_element_type=F32)
            for s in range(n_dev):
                osum[s, e * load:(e + 1) * load, :] = out[s * load:(s + 1) * load]
        for s in range(n_dev):
            rhs = osum[s].astype(BF16)
            acc = jnp.dot(coef[m, 0, s], rhs, preferred_element_type=F32)
            acc += jnp.dot(coef[m, 1, s], rhs, preferred_element_type=F32)
            acc += jnp.dot(coef[m, 2, s], rhs, preferred_element_type=F32)
            part[slot, s % 2, s // 2] = acc
        core_part(k).start()

    def down_next(k):
        for p in range(2):
            q = 2 * k + p + n_slot_w2

            @pl.when(q < 2 * n_step)
            def _():
                w2_copy(q).start()

    def down(m, k):
        down_wait(k)
        down_math(m, k)
        down_next(k)

    def core_part(k):
        ps, ds = lax.rem(k, n_slot_p), lax.rem(k, n_slot_d)
        return remote(part.at[ps, other], dbuf.at[ds], d_send.at[ps], d_recv.at[ds], partner)

    def far_part(k, d):
        s, r = lax.rem(k, n_slot_c), lax.rem(k, n_slot_r)
        return remote(cbuf.at[s, far_c, pl.ds(d * half, half)], rbuf.at[r, d], r_send.at[s, d], r_recv.at[r, d], side[d])

    def near_part(k, d, h):
        s, f = lax.rem(k, n_slot_c), lax.rem(k, n_slot_f)
        return remote(cbuf.at[s, (right_c, left_c)[d], pl.ds(h * half, half)], fbuf.at[f, d, pl.ds(h * half, half)],
                      f_send.at[s, d, h], f_recv.at[f, d, h], side[d])

    def drain_sends(k):
        for d in range(2):
            far_part(k, d).wait_send()
            near_part(k, d, 0).wait_send()
            near_part(k, d, 1).wait_send()

    def stage2(k):
        @pl.when(k >= n_slot_c)
        def _():
            drain_sends(k - n_slot_c)
        core_part(k).wait_recv()
        s, ds, ps = lax.rem(k, n_slot_c), lax.rem(k, n_slot_d), lax.rem(k, n_slot_p)
        for c in range(n_chip):
            cbuf[s, c] = part[ps, core, c] + dbuf[ds, c]
        for d in range(2):
            far_part(k, d).start()
        for d in range(2):
            near_part(k, d, 1 - d).start()

    def stage3(k):
        s = lax.rem(k, n_slot_c)
        for d in range(2):
            far_part(k, d).wait_recv()
            c = (right_c, left_c)[d]
            cbuf[s, c, d * half:(d + 1) * half] = cbuf[s, c, d * half:(d + 1) * half] + rbuf[lax.rem(k, n_slot_r), d]
            near_part(k, d, d).start()

    def stage4(k, m, y_ref):
        s, f = lax.rem(k, n_slot_c), lax.rem(k, n_slot_f)

        for d in range(2):
            for h in range(2):
                near_part(k, d, h).wait_recv()
        col = pl.multiple_of(lax.rem(k, n_col) * CW, CW)
        x_own = xall[m, chip, pl.ds(pl.multiple_of(core * tok, 16), tok), pl.ds(col, CW)].astype(F32)
        y_ref[:, pl.ds(col, CW)] = (x_own + (cbuf[s, chip] + fbuf[f, 0] + fbuf[f, 1])).astype(BF16)

    def stage4_at(k):
        @pl.when((k >= 0) & (k < n_col))
        def _():
            stage4(k, 0, ya_ref)

        @pl.when(k >= n_col)
        def _():
            stage4(k, 1, yb_ref)

    barrier = pltpu.get_barrier_semaphore()
    for i in range(1, n_dev):
        pl.semaphore_signal(barrier, inc=1, device_id={'expert': lax.rem(me + i, n_dev)}, device_id_type=pl.DeviceIdType.MESH)
    own_load(0).start()
    route_loads = [pltpu.make_async_copy(src, dst, route_sem.at[i]) for i, (src, dst) in enumerate(
        ((idx_a_hbm, idx_v.at[0]), (gate_a_hbm, gate_v.at[0]), (idx_b_hbm, idx_v.at[1]), (gate_b_hbm, gate_v.at[1])))]
    for copy in route_loads:
        copy.start()
    own_load(1).start()
    for copy in route_loads:
        copy.wait()
    for m in range(2):
        meta[m, me, 0:k_top] = idx_v[m].astype(F32)
        meta[m, me, k_top:8] = jnp.zeros((8 - k_top, tok), F32)
        meta[m, me, 8:8 + k_top] = gate_v[m]
        meta[m, me, 8 + k_top:16] = jnp.zeros((8 - k_top, tok), F32)
    own_load(0).wait()
    pl.semaphore_wait(barrier, n_dev - 1)

    right, left = side
    far = far_c * 2 + core

    def meta_copy(m, dev, i, to):
        return remote(meta.at[m, dev], meta.at[m, dev], meta_send.at[m, i], meta_recv.at[m, i], to)

    def meta_sends(m):
        return [meta_copy(m, me, 0, right), meta_copy(m, me, 1, left), meta_copy(m, me, 2, far), meta_copy(m, me, 3, partner),
                meta_copy(m, left, 4, partner), meta_copy(m, right, 5, partner), meta_copy(m, far, 6, partner)]

    def meta_arrivals(m):
        return [meta_copy(m, left, 0, right), meta_copy(m, right, 1, left), meta_copy(m, far, 2, far)] + [
            meta_copy(m, c * 2 + other, 3 + i, partner) for i, c in enumerate((chip, left_c, right_c, far_c))]

    def meta_start(m):
        for copy in meta_sends(m)[:4]:
            copy.start()

    def meta_share(m):
        for i in range(3):
            meta_arrivals(m)[i].wait_recv()
            meta_sends(m)[4 + i].start()

    def meta_end(m):
        for copy in meta_arrivals(m)[3:]:
            copy.wait_recv()

    meta_start(0)
    own_send(0, 0, 0).start()
    own_send(0, 1, 1).start()
    meta_start(1)
    own_send(0, 0, 1).start()
    own_send(0, 1, 0).start()
    for q in range(n_slot_w1):
        w1_copy(jnp.int32(q)).start()
    for q in range(n_slot_w2):
        w2_copy(jnp.int32(q)).start()
    pick_f[...] = jnp.zeros_like(pick_f)
    for s in range(n_dev):
        osum[s, n_exp * load:lanes] = jnp.zeros((lanes - n_exp * load, CW), F32)
    to_partner(0, 0).start()
    meta_share(0)
    meta_end(0)
    routing(0)
    relay_first(0)
    own_load(1).wait()
    own_send(1, 0, 0).start()
    own_send(1, 1, 1).start()
    own_send(1, 0, 1).start()
    own_send(1, 1, 0).start()
    meta_share(1)
    meta_end(1)
    routing(1)
    from_partner(0, 0).wait_recv()
    gather(0, chip)
    relay_second(0)
    from_partner(0, 1).wait_recv()
    gather(0, right_c)
    from_partner(0, 2).wait_recv()
    gather(0, left_c)
    relay_far(0)
    to_partner(1, 0).start()
    far_from_partner(0)
    gather(0, far_c)

    def up_a(e, carry):
        up(0, e)

        @pl.when(e == 3)
        def _():
            relay_first(1)

        @pl.when(e == 6)
        def _():
            relay_second(1)
        return carry

    lax.fori_loop(0, n_exp, up_a, 0)

    down(0, jnp.int32(0))
    for i, c in ((0, chip), (1, right_c), (2, left_c)):
        from_partner(1, i).wait_recv()
        gather(1, c)
    stage2(jnp.int32(0))
    relay_far(1)
    down(0, jnp.int32(1))
    far_from_partner(1)
    gather(1, far_c)
    up(1, jnp.int32(0))
    stage2(jnp.int32(1))

    def first_steps(k, carry):
        down(0, k)
        stage3(k - 2)
        up(1, k - 1)
        stage4_at(k - 3)
        stage2(k)
        return carry

    lax.fori_loop(2, n_col, first_steps, 0)

    for e in range(n_col - 1, n_exp):
        up(1, jnp.int32(e))

    def last_steps(k, carry):
        down(1, k)
        stage3(k - 2)
        stage4_at(k - 3)
        stage2(k)
        return carry

    lax.fori_loop(n_col, n_step, last_steps, 0)
    last = jnp.int32(n_step - 1)
    stage3(last - 1)
    stage4(last - 2, 1, yb_ref)
    stage3(last)
    stage4(last - 1, 1, yb_ref)
    stage4(last, 1, yb_ref)

    for m in range(2):
        for copy in meta_sends(m):
            copy.wait_send()
    for m in range(2):
        for d in range(2):
            for h in range(2):
                own_send(m, d, h).wait_send()
            forward(m, d).wait_send()
        for i in range(3):
            to_partner(m, i).wait_send()
        for d in range(2):
            far_to_partner(m, d, core).wait_send()
    for k in range(n_step - n_slot_p, n_step):
        core_part(jnp.int32(k)).wait_send()
    for k in range(n_step - n_slot_c, n_step):
        drain_sends(jnp.int32(k))


def write_out(ya_vmem, yb_vmem, ya_hbm, yb_hbm, sem):
    copies = [pltpu.make_async_copy(src, dst, sem.at[i]) for i, (src, dst) in enumerate(((ya_vmem, ya_hbm), (yb_vmem, yb_hbm)))]
    for copy in copies:
        copy.start()
    for copy in copies:
        copy.wait()


def solution(mesh):
    n_dev = mesh.shape['expert']
    row_spec = P(('data', 'expert'), None)
    weight_spec = P('expert', None, None)

    def device_fn(x_a, idx_a, gate_a, x_b, idx_b, gate_b, w_up, w_down):
        tok, d_model = x_a.shape
        k_top = idx_a.shape[1]
        n_exp, _, d_ff = w_up.shape
        n_chip = n_dev // 2
        cap = tok * k_top // n_exp
        load = 2 * tok * k_top // (n_exp * n_dev)
        lanes = -(-n_exp * load // 128) * 128
        rows = n_dev * load
        half = tok // 2
        dims = (n_dev, n_chip, tok, k_top, d_model, d_ff, n_exp, load, cap)
        dma = pltpu.SemaphoreType.DMA
        any_spec = pl.BlockSpec(memory_space=pl.ANY)
        vmem_spec = pl.BlockSpec(memory_space=pltpu.VMEM)
        scratch = [
            pltpu.VMEM((2, n_chip, 2 * tok, d_model), BF16),
            pltpu.VMEM((n_exp, rows, d_model), BF16),
            pltpu.VMEM((2, n_exp, rows, d_ff), BF16),
            pltpu.VMEM((5, d_model // 2, d_ff), BF16),
            pltpu.VMEM((3, n_exp // 2, d_ff, CW), BF16),
            pltpu.VMEM((2, 3, n_dev, tok, lanes), BF16),
            pltpu.VMEM((2, n_chip, 2 * n_exp * load, 2 * tok), BF16),
            pltpu.VMEM((2 * n_exp * load, 2 * tok), F32),
            pltpu.VMEM((2, k_top, tok), jnp.int32),
            pltpu.VMEM((2, k_top, tok), F32),
            pltpu.VMEM((2, n_dev, 16, tok), F32),
            pltpu.VMEM((n_dev, lanes, CW), F32),
            pltpu.VMEM((2, 2, n_chip, tok, CW), F32),
            pltpu.VMEM((2, n_chip, tok, CW), F32),
            pltpu.VMEM((3, n_chip, tok, CW), F32),
            pltpu.VMEM((4, 2, half, CW), F32),
            pltpu.VMEM((5, 2, tok, CW), F32),
            dma((2, 7)), dma((2, 7)), dma((4,)), dma((2,)),
            dma((2, 2, 2)), dma((2, 2, 3)), dma((2, 2)),
            dma((2, 5)), dma((2, 5)),
            dma((5,)), dma((3,)),
            dma((2,)), dma((2,)),
            dma((3, 2)), dma((4, 2)),
            dma((3, 2, 2)), dma((5, 2, 2)),
        ]
        y_a, y_b = pl.pallas_call(
            functools.partial(moe_kernel, dims),
            out_shape=(pltpu.VMEM(x_a.shape, BF16), pltpu.VMEM(x_b.shape, BF16)),
            in_specs=[any_spec] * 8,
            out_specs=(vmem_spec, vmem_spec),
            scratch_shapes=scratch,
            compiler_params=pltpu.CompilerParams(collective_id=0, has_side_effects=True, vmem_limit_bytes=65994752),
        )(idx_a.T, gate_a.T, idx_b.T, gate_b.T, x_a, x_b, w_up, w_down)
        return pl.pallas_call(
            write_out,
            out_shape=(jax.ShapeDtypeStruct(x_a.shape, BF16), jax.ShapeDtypeStruct(x_b.shape, BF16)),
            in_specs=[vmem_spec] * 2,
            out_specs=(any_spec, any_spec),
            scratch_shapes=[dma((2,))],
        )(pltpu.with_memory_space_constraint(y_a, pltpu.VMEM), pltpu.with_memory_space_constraint(y_b, pltpu.VMEM))

    return jax.shard_map(device_fn, mesh=mesh, in_specs=(row_spec, row_spec, row_spec, row_spec, row_spec, row_spec, weight_spec, weight_spec), out_specs=(row_spec, row_spec), check_vma=False)
```

```python
import functools

import jax
import jax.numpy as jnp
from jax import lax
from jax.experimental import pallas as pl
from jax.experimental.pallas import tpu as pltpu
from jax.sharding import PartitionSpec as P

F32 = jnp.float32
BF16 = jnp.bfloat16
CW = 256
TW = 768


def moe_kernel(dims, idx_a_hbm, gate_a_hbm, idx_b_hbm, gate_b_hbm, xa_hbm, xb_hbm, wu_hbm, wd_hbm, ya_ref, yb_ref,
               xall, buf, hid, w1, w2, coef, pick, pick_f, idx_v, gate_v, meta, osum, part, dbuf, cbuf, rbuf, fbuf,
               meta_send, meta_recv, route_sem, x_sem, ag_send, ag_recv, fwd_send, core_send, core_recv,
               w1_sem, w2_sem, d_send, d_recv, r_send, r_recv, f_send, f_recv):
    n_dev, n_chip, tok, k_top, d_model, d_ff, n_exp, load, cap = dims
    lanes = coef.shape[-1]
    rows = n_dev * load
    half = tok // 2
    pair = 2 * load
    n_col = d_model // CW
    n_step = 2 * n_col
    bounds = [(t, min(TW, d_ff - t)) for t in range(0, d_ff, TW)]
    n_slot_p, n_slot_d, n_slot_c, n_slot_f = part.shape[0], dbuf.shape[0], cbuf.shape[0], fbuf.shape[0]
    n_slot_r = rbuf.shape[0]
    e_half = n_exp // 2
    n_slot_w1, n_slot_w2 = w1.shape[0], w2.shape[0]

    me = lax.axis_index('expert')
    chip, core = me // 2, lax.rem(me, 2)
    other = 1 - core
    right_c, left_c, far_c = lax.rem(chip + 1, n_chip), lax.rem(chip + n_chip - 1, n_chip), lax.rem(chip + 2, n_chip)
    partner = chip * 2 + other
    side = (right_c * 2 + core, left_c * 2 + core)

    def remote(src, dst, send, recv, dev):
        return pltpu.make_async_remote_copy(src_ref=src, dst_ref=dst, send_sem=send, recv_sem=recv,
                                            device_id={'expert': dev}, device_id_type=pl.DeviceIdType.MESH)

    def w1_copy(q):
        slot = lax.rem(q, n_slot_w1)
        return pltpu.make_async_copy(wu_hbm.at[lax.rem(q // 2, n_exp), pl.ds(lax.rem(q, 2) * (d_model // 2), d_model // 2)],
                                     w1.at[slot], w1_sem.at[slot])

    def w2_copy(q):
        step, part_id = q // 2, lax.rem(q, 2)
        col = pl.multiple_of(lax.rem(step, n_col) * CW, CW)
        slot = lax.rem(q, n_slot_w2)
        return pltpu.make_async_copy(wd_hbm.at[pl.ds(part_id * e_half, e_half), :, pl.ds(col, CW)], w2.at[slot], w2_sem.at[slot])

    def block(m, c, r0=0, n=tok, k=None):
        k = core if k is None else k
        return xall.at[m, c, pl.ds(pl.multiple_of(k * tok + r0, 16), n), :]

    def own_load(m):
        return pltpu.make_async_copy((xa_hbm, xb_hbm)[m], block(m, chip), x_sem.at[m])

    def own_send(m, d, h):
        ref = block(m, chip, h * half, half)
        return remote(ref, ref, ag_send.at[m, d, h], ag_recv.at[m, d, h], side[d])

    def own_arrival(m, d, h):
        ref = block(m, (left_c, right_c)[d], h * half, half)
        return remote(ref, ref, ag_send.at[m, d, h], ag_recv.at[m, d, h], side[d])

    def forward(m, d):
        ref = block(m, (left_c, right_c)[d], d * half, half)
        return remote(ref, ref, fwd_send.at[m, d], ag_recv.at[m, d, 2], side[d])

    def far_arrival(m, d):
        ref = block(m, far_c, d * half, half)
        return remote(ref, ref, fwd_send.at[m, d], ag_recv.at[m, d, 2], side[d])

    def to_partner(m, i):
        ref = block(m, (chip, right_c, left_c, far_c)[i])
        return remote(ref, ref, core_send.at[m, i], core_recv.at[m, i], partner)

    def far_to_partner(m, d, k):
        ref = block(m, far_c, d * half, half, k=k)
        return remote(ref, ref, core_send.at[m, 3 + d], core_recv.at[m, 3 + d], partner)

    def far_from_partner(m):
        for d in range(2):
            far_to_partner(m, d, other).wait_recv()

    def from_partner(m, i):
        ref = block(m, (chip, right_c, left_c, far_c)[i], k=other)
        return remote(ref, ref, core_send.at[m, i], core_recv.at[m, i], partner)

    def relay_first(m):
        for d in range(2):
            own_arrival(m, d, d).wait_recv()
            forward(m, d).start()

    def relay_second(m):
        own_arrival(m, 1, 0).wait_recv()
        to_partner(m, 1).start()
        own_arrival(m, 0, 1).wait_recv()
        to_partner(m, 2).start()

    def relay_far(m):
        for d in range(2):
            far_arrival(m, d).wait_recv()
            far_to_partner(m, d, core).start()

    def routing(m):
        lane = lax.broadcasted_iota(jnp.int32, (1, lanes), 1)
        lane_e = jnp.where(lane < n_exp * load, me * n_exp + lane // load, -1).astype(F32)
        lane_r = lax.rem(lane, load).astype(F32)
        row_id = lax.broadcasted_iota(jnp.int32, (tok, tok), 0)
        col_id = lax.broadcasted_iota(jnp.int32, (tok, tok), 1)
        below = jnp.where(col_id < row_id, 1.0, 0.0).astype(BF16)

        def one_source(s, before):
            facts = jnp.concatenate([meta[m, s], jnp.zeros((tok - meta.shape[2], tok), F32)], axis=0).T
            hit = jnp.zeros((tok, lanes), F32)
            gate = jnp.zeros((tok, lanes), F32)
            for j in range(k_top):
                same = facts[:, j:j + 1] == lane_e
                hit = jnp.where(same, 1.0, hit)
                gate = jnp.where(same, facts[:, 8 + j:9 + j], gate)
            rank = jnp.dot(below, hit.astype(BF16), preferred_element_type=F32)
            keep = (hit > 0.0) & (rank == lane_r) & (before + rank < float(cap))
            gate = jnp.where(keep, gate, 0.0)
            hi = (gate * 0.9921875).astype(BF16)
            rest = gate - hi.astype(F32)
            mid = rest.astype(BF16)
            low = (rest - mid.astype(F32)).astype(BF16)
            coef[m, 0, s] = hi
            coef[m, 1, s] = mid
            coef[m, 2, s] = low
            chosen = jnp.where(keep, 1.0, 0.0).T
            return before + jnp.sum(hit, axis=0, keepdims=True), chosen

        before = jnp.zeros((1, lanes), F32)
        for c in range(n_chip):
            for k in range(2):
                before, chosen = one_source(2 * c + k, before)
                for e in range(n_exp):
                    pick_f[e * pair + k * load:e * pair + (k + 1) * load, k * tok:(k + 1) * tok] = chosen[e * load:(e + 1) * load]
            pick[m, c] = pick_f[...].astype(BF16)

    def gather(m, c):
        for n in range(0, d_model, 512):
            got = jnp.dot(pick[m, c], xall[m, c, :, n:n + 512], preferred_element_type=F32).astype(BF16)
            for e in range(n_exp):
                buf[e, pl.ds(pl.multiple_of(c * pair, 16), pair), n:n + 512] = got[e * pair:(e + 1) * pair]

    def up_wait(m, e):
        for h in range(2):
            w1_copy(2 * (m * n_exp + e) + h).wait()

    def up_math(m, e):
        q = 2 * (m * n_exp + e)
        depth = d_model // 2
        for lo, width in bounds:
            acc = jnp.dot(buf[e, :, 0:depth], w1[lax.rem(q, n_slot_w1), :, lo:lo + width], preferred_element_type=F32)
            acc += jnp.dot(buf[e, :, depth:], w1[lax.rem(q + 1, n_slot_w1), :, lo:lo + width], preferred_element_type=F32)
            hid[m, e, :, lo:lo + width] = jax.nn.gelu(acc, approximate=True).astype(BF16)

    def up_next(m, e):
        for h in range(2):
            nxt = 2 * (m * n_exp + e) + h + n_slot_w1

            @pl.when(nxt < 4 * n_exp)
            def _():
                w1_copy(nxt).start()

    def up(m, e):
        up_wait(m, e)
        up_math(m, e)
        up_next(m, e)

    def down_wait(k):
        for p in range(2):
            w2_copy(2 * k + p).wait()

        @pl.when(k >= n_slot_p)
        def _():
            core_part(k - n_slot_p).wait_send()

    def down_math(m, k):
        slot = lax.rem(k, n_slot_p)
        for e in range(n_exp):
            out = jnp.dot(hid[m, e], w2[lax.rem(2 * k + e // e_half, n_slot_w2), e % e_half], preferred_element_type=F32)
            for s in range(n_dev):
                osum[s, e * load:(e + 1) * load, :] = out[s * load:(s + 1) * load]
        for s in range(n_dev):
            rhs = osum[s].astype(BF16)
            acc = jnp.dot(coef[m, 0, s], rhs, preferred_element_type=F32)
            acc += jnp.dot(coef[m, 1, s], rhs, preferred_element_type=F32)
            acc += jnp.dot(coef[m, 2, s], rhs, preferred_element_type=F32)
            part[slot, s % 2, s // 2] = acc
        core_part(k).start()

    def down_next(k):
        for p in range(2):
            q = 2 * k + p + n_slot_w2

            @pl.when(q < 2 * n_step)
            def _():
                w2_copy(q).start()

    def down(m, k):
        down_wait(k)
        down_math(m, k)
        down_next(k)

    def core_part(k):
        ps, ds = lax.rem(k, n_slot_p), lax.rem(k, n_slot_d)
        return remote(part.at[ps, other], dbuf.at[ds], d_send.at[ps], d_recv.at[ds], partner)

    def far_part(k, d):
        s, r = lax.rem(k, n_slot_c), lax.rem(k, n_slot_r)
        return remote(cbuf.at[s, far_c, pl.ds(d * half, half)], rbuf.at[r, d], r_send.at[s, d], r_recv.at[r, d], side[d])

    def near_part(k, d, h):
        s, f = lax.rem(k, n_slot_c), lax.rem(k, n_slot_f)
        return remote(cbuf.at[s, (right_c, left_c)[d], pl.ds(h * half, half)], fbuf.at[f, d, pl.ds(h * half, half)],
                      f_send.at[s, d, h], f_recv.at[f, d, h], side[d])

    def drain_sends(k):
        for d in range(2):
            far_part(k, d).wait_send()
            near_part(k, d, 0).wait_send()
            near_part(k, d, 1).wait_send()

    def stage2(k):
        @pl.when(k >= n_slot_c)
        def _():
            drain_sends(k - n_slot_c)
        core_part(k).wait_recv()
        s, ds, ps = lax.rem(k, n_slot_c), lax.rem(k, n_slot_d), lax.rem(k, n_slot_p)
        for c in range(n_chip):
            cbuf[s, c] = part[ps, core, c] + dbuf[ds, c]
        for d in range(2):
            far_part(k, d).start()
        for d in range(2):
            near_part(k, d, 1 - d).start()

    def stage3(k):
        s = lax.rem(k, n_slot_c)
        for d in range(2):
            far_part(k, d).wait_recv()
            c = (right_c, left_c)[d]
            cbuf[s, c, d * half:(d + 1) * half] = cbuf[s, c, d * half:(d + 1) * half] + rbuf[lax.rem(k, n_slot_r), d]
            near_part(k, d, d).start()

    def stage4(k, m, y_ref):
        s, f = lax.rem(k, n_slot_c), lax.rem(k, n_slot_f)

        for d in range(2):
            for h in range(2):
                near_part(k, d, h).wait_recv()
        col = pl.multiple_of(lax.rem(k, n_col) * CW, CW)
        x_own = xall[m, chip, pl.ds(pl.multiple_of(core * tok, 16), tok), pl.ds(col, CW)].astype(F32)
        y_ref[:, pl.ds(col, CW)] = (x_own + (cbuf[s, chip] + fbuf[f, 0] + fbuf[f, 1])).astype(BF16)

    def stage4_at(k):
        @pl.when((k >= 0) & (k < n_col))
        def _():
            stage4(k, 0, ya_ref)

        @pl.when(k >= n_col)
        def _():
            stage4(k, 1, yb_ref)

    barrier = pltpu.get_barrier_semaphore()
    for i in range(1, n_dev):
        pl.semaphore_signal(barrier, inc=1, device_id={'expert': lax.rem(me + i, n_dev)}, device_id_type=pl.DeviceIdType.MESH)
    own_load(0).start()
    route_loads = [pltpu.make_async_copy(src, dst, route_sem.at[i]) for i, (src, dst) in enumerate(
        ((idx_a_hbm, idx_v.at[0]), (gate_a_hbm, gate_v.at[0]), (idx_b_hbm, idx_v.at[1]), (gate_b_hbm, gate_v.at[1])))]
    for copy in route_loads:
        copy.start()
    own_load(1).start()
    for copy in route_loads:
        copy.wait()
    for m in range(2):
        meta[m, me, 0:k_top] = idx_v[m].astype(F32)
        meta[m, me, k_top:8] = jnp.zeros((8 - k_top, tok), F32)
        meta[m, me, 8:8 + k_top] = gate_v[m]
        meta[m, me, 8 + k_top:16] = jnp.zeros((8 - k_top, tok), F32)
    own_load(0).wait()
    pl.semaphore_wait(barrier, n_dev - 1)

    right, left = side
    far = far_c * 2 + core

    def meta_copy(m, dev, i, to):
        return remote(meta.at[m, dev], meta.at[m, dev], meta_send.at[m, i], meta_recv.at[m, i], to)

    def meta_sends(m):
        return [meta_copy(m, me, 0, right), meta_copy(m, me, 1, left), meta_copy(m, me, 2, far), meta_copy(m, me, 3, partner),
                meta_copy(m, left, 4, partner), meta_copy(m, right, 5, partner), meta_copy(m, far, 6, partner)]

    def meta_arrivals(m):
        return [meta_copy(m, left, 0, right), meta_copy(m, right, 1, left), meta_copy(m, far, 2, far)] + [
            meta_copy(m, c * 2 + other, 3 + i, partner) for i, c in enumerate((chip, left_c, right_c, far_c))]

    def meta_start(m):
        for copy in meta_sends(m)[:4]:
            copy.start()

    def meta_share(m):
        for i in range(3):
            meta_arrivals(m)[i].wait_recv()
            meta_sends(m)[4 + i].start()

    def meta_end(m):
        for copy in meta_arrivals(m)[3:]:
            copy.wait_recv()

    meta_start(0)
    own_send(0, 0, 0).start()
    own_send(0, 1, 1).start()
    meta_start(1)
    own_send(0, 0, 1).start()
    own_send(0, 1, 0).start()
    for q in range(n_slot_w1):
        w1_copy(jnp.int32(q)).start()
    for q in range(n_slot_w2):
        w2_copy(jnp.int32(q)).start()
    pick_f[...] = jnp.zeros_like(pick_f)
    for s in range(n_dev):
        osum[s, n_exp * load:lanes] = jnp.zeros((lanes - n_exp * load, CW), F32)
    to_partner(0, 0).start()
    meta_share(0)
    meta_end(0)
    routing(0)
    relay_first(0)
    own_load(1).wait()
    own_send(1, 0, 0).start()
    own_send(1, 1, 1).start()
    own_send(1, 0, 1).start()
    own_send(1, 1, 0).start()
    meta_share(1)
    meta_end(1)
    routing(1)
    from_partner(0, 0).wait_recv()
    gather(0, chip)
    relay_second(0)
    from_partner(0, 1).wait_recv()
    gather(0, right_c)
    from_partner(0, 2).wait_recv()
    gather(0, left_c)
    relay_far(0)
    to_partner(1, 0).start()
    far_from_partner(0)
    gather(0, far_c)

    def up_a(e, carry):
        up(0, e)

        @pl.when(e == 3)
        def _():
            relay_first(1)

        @pl.when(e == 6)
        def _():
            relay_second(1)
        return carry

    lax.fori_loop(0, n_exp, up_a, 0)

    down(0, jnp.int32(0))
    for i, c in ((0, chip), (1, right_c), (2, left_c)):
        from_partner(1, i).wait_recv()
        gather(1, c)
    stage2(jnp.int32(0))
    relay_far(1)
    down(0, jnp.int32(1))
    far_from_partner(1)
    gather(1, far_c)
    up(1, jnp.int32(0))
    stage2(jnp.int32(1))

    def first_steps(k, carry):
        down(0, k)
        stage3(k - 2)
        up(1, k - 1)
        stage4_at(k - 3)
        stage2(k)
        return carry

    lax.fori_loop(2, n_col, first_steps, 0)

    for e in range(n_col - 1, n_exp):
        up(1, jnp.int32(e))

    def last_steps(k, carry):
        down(1, k)
        stage3(k - 2)
        stage4_at(k - 3)
        stage2(k)
        return carry

    lax.fori_loop(n_col, n_step, last_steps, 0)
    last = jnp.int32(n_step - 1)
    stage3(last - 1)
    stage4(last - 2, 1, yb_ref)
    stage3(last)
    stage4(last - 1, 1, yb_ref)
    stage4(last, 1, yb_ref)

    for m in range(2):
        for copy in meta_sends(m):
            copy.wait_send()
    for m in range(2):
        for d in range(2):
            for h in range(2):
                own_send(m, d, h).wait_send()
            forward(m, d).wait_send()
        for i in range(3):
            to_partner(m, i).wait_send()
        for d in range(2):
            far_to_partner(m, d, core).wait_send()
    for k in range(n_step - n_slot_p, n_step):
        core_part(jnp.int32(k)).wait_send()
    for k in range(n_step - n_slot_c, n_step):
        drain_sends(jnp.int32(k))


def write_out(ya_vmem, yb_vmem, ya_hbm, yb_hbm, sem):
    copies = [pltpu.make_async_copy(src, dst, sem.at[i]) for i, (src, dst) in enumerate(((ya_vmem, ya_hbm), (yb_vmem, yb_hbm)))]
    for copy in copies:
        copy.start()
    for copy in copies:
        copy.wait()


def solution(mesh):
    n_dev = mesh.shape['expert']
    row_spec = P(('data', 'expert'), None)
    weight_spec = P('expert', None, None)

    def device_fn(x_a, idx_a, gate_a, x_b, idx_b, gate_b, w_up, w_down):
        tok, d_model = x_a.shape
        k_top = idx_a.shape[1]
        n_exp, _, d_ff = w_up.shape
        n_chip = n_dev // 2
        cap = tok * k_top // n_exp
        load = 2 * tok * k_top // (n_exp * n_dev)
        lanes = -(-n_exp * load // 128) * 128
        rows = n_dev * load
        half = tok // 2
        dims = (n_dev, n_chip, tok, k_top, d_model, d_ff, n_exp, load, cap)
        dma = pltpu.SemaphoreType.DMA
        any_spec = pl.BlockSpec(memory_space=pl.ANY)
        vmem_spec = pl.BlockSpec(memory_space=pltpu.VMEM)
        scratch = [
            pltpu.VMEM((2, n_chip, 2 * tok, d_model), BF16),
            pltpu.VMEM((n_exp, rows, d_model), BF16),
            pltpu.VMEM((2, n_exp, rows, d_ff), BF16),
            pltpu.VMEM((5, d_model // 2, d_ff), BF16),
            pltpu.VMEM((3, n_exp // 2, d_ff, CW), BF16),
            pltpu.VMEM((2, 3, n_dev, tok, lanes), BF16),
            pltpu.VMEM((2, n_chip, 2 * n_exp * load, 2 * tok), BF16),
            pltpu.VMEM((2 * n_exp * load, 2 * tok), F32),
            pltpu.VMEM((2, k_top, tok), jnp.int32),
            pltpu.VMEM((2, k_top, tok), F32),
            pltpu.VMEM((2, n_dev, 16, tok), F32),
            pltpu.VMEM((n_dev, lanes, CW), F32),
            pltpu.VMEM((2, 2, n_chip, tok, CW), F32),
            pltpu.VMEM((2, n_chip, tok, CW), F32),
            pltpu.VMEM((3, n_chip, tok, CW), F32),
            pltpu.VMEM((4, 2, half, CW), F32),
            pltpu.VMEM((5, 2, tok, CW), F32),
            dma((2, 7)), dma((2, 7)), dma((4,)), dma((2,)),
            dma((2, 2, 2)), dma((2, 2, 3)), dma((2, 2)),
            dma((2, 5)), dma((2, 5)),
            dma((5,)), dma((3,)),
            dma((2,)), dma((2,)),
            dma((3, 2)), dma((4, 2)),
            dma((3, 2, 2)), dma((5, 2, 2)),
        ]
        y_a, y_b = pl.pallas_call(
            functools.partial(moe_kernel, dims),
            out_shape=(pltpu.VMEM(x_a.shape, BF16), pltpu.VMEM(x_b.shape, BF16)),
            in_specs=[any_spec] * 8,
            out_specs=(vmem_spec, vmem_spec),
            scratch_shapes=scratch,
            compiler_params=pltpu.CompilerParams(collective_id=0, has_side_effects=True, vmem_limit_bytes=65994752),
        )(idx_a.T, gate_a.T, idx_b.T, gate_b.T, x_a, x_b, w_up, w_down)
        return pl.pallas_call(
            write_out,
            out_shape=(jax.ShapeDtypeStruct(x_a.shape, BF16), jax.ShapeDtypeStruct(x_b.shape, BF16)),
            in_specs=[vmem_spec] * 2,
            out_specs=(any_spec, any_spec),
            scratch_shapes=[dma((2,))],
        )(pltpu.with_memory_space_constraint(y_a, pltpu.VMEM), pltpu.with_memory_space_constraint(y_b, pltpu.VMEM))

    return jax.shard_map(device_fn, mesh=mesh, in_specs=(row_spec, row_spec, row_spec, row_spec, row_spec, row_spec, weight_spec, weight_spec), out_specs=(row_spec, row_spec), check_vma=False)
```
